32 devices in a mesh: group: 2 (over x), serve: 8 (over z, y), tensor: 2 (over core).
Axes of the slice: x: 2, y: 2, z: 4, core: 2. Of those that a mesh axis runs over, the one named last changes fastest.
Arguments:
- tokens: bfloat16 [2048, 8192], P(('group', 'serve'), 'tensor'), parts along dimension 0, may hold values from -70 to 70
- query_weight: bfloat16 [8192, 512], P(None, 'tensor'), may hold values from -0.0625 to 0.0625
- key_value_weight: bfloat16 [8192, 256], P(None, 'tensor'), may hold values from -0.0625 to 0.0625
- output_weight: bfloat16 [512, 8192], P('tensor'), may hold values from -0.25 to 0.25
- adapter_down_maps: bfloat16 [32, 48, 8192], P(('group', 'serve'), None, 'tensor'), parts along dimension 0, may hold values from -0.0625 to 0.0625
- adapter_query_up: bfloat16 [32, 16, 512], P(('group', 'serve'), None, 'tensor'), parts along dimension 0, may hold values from -1.5 to 1.5
- adapter_key_value_up: bfloat16 [32, 16, 256], P(('group', 'serve'), None, 'tensor'), parts along dimension 0, may hold values from -1.5 to 1.5
- adapter_output_down: bfloat16 [32, 16, 512], P(('group', 'serve'), None, 'tensor'), parts along dimension 0, may hold values from -0.25 to 0.25
- adapter_output_up: bfloat16 [32, 16, 8192], P(('group', 'serve'), None, 'tensor'), parts along dimension 0, may hold values from -1.5 to 1.5
- request_adapter: int32 [16], P('group'), parts along dimension 0, may hold values from 0 to 15, as said below
- adapter_pool_row: int32 [32], P('group'), parts along dimension 0, may hold values from 0 to 15, as said below
- lengths: int32 [16], P(('group', 'serve')), parts along dimension 0, may hold values from 16 to 128
Outputs:
- attention_out: bfloat16 [2048, 8192], P(('group', 'serve'), 'tensor'), parts along dimension 0
The draws below stay inside these ranges and needn't reach their ends.
There are 2 independent parts, one for each index of `group`. The reference program is written for one: setup_inputs(seed, part) draws one part's arguments, and reference() takes and returns one part's arrays. A program takes and returns all parts, laid end to end along the dimension named above; an argument that names none is the same for every part. Nothing has to cross between parts.
Inputs may be any that keep to these rules, and one draw needn't show every extreme that they name: Grouping requests by adapter_pool_row[request_adapter[r]] // 2, no group holds more than 4 requests, and some group holds exactly 4. `adapter_pool_row`: each value appears once.
All inputs are finite; a program needn't handle non-finite values.
Results may differ from the reference program's by a relative error of at most 0.012.
The reference program's roundings to bfloat16 on the way count: a program that leaves them out, or rounds other values in their place, can miss the bound.
Values may be sent and summed in bfloat16 or wider, within the bound.
A program may use at most 128 MiB of HBM per device.

```python
import jax
import jax.numpy as jnp
from jax import lax

MODEL_WIDTH = 8192
HEAD_SIZE = 128
ADAPTER_RANK = 16
QUERY_HEADS = 4
CAP = 4
LEN = 128
ADP_DEV = 2
REQUESTS = 8
ADAPTER_POOL = 16
TOKENS = 1024


def draw_tokens(key, part):
    key_base = jax.random.fold_in(jax.random.fold_in(key, 11), 0)
    base_draw = jnp.clip(jax.random.normal(key_base, (TOKENS, MODEL_WIDTH), jnp.float32), -5.0, 5.0)
    return base_draw.astype(jnp.bfloat16)


def placement_draw(key):
    key_hot, key_seat, key_mix, key_local, key_slot = jax.random.split(jax.random.fold_in(key, 23), 5)
    seats_total = REQUESTS * CAP
    hot_owner = jax.random.randint(key_hot, (), 0, REQUESTS)
    seat_index = jnp.arange(seats_total, dtype=jnp.int32)
    seat_owner = seat_index // CAP
    scores = jax.random.permutation(key_seat, seats_total).astype(jnp.int32)
    scores = jnp.where(seat_owner == hot_owner, -1 - seat_index % CAP, scores)
    taken = jnp.argsort(scores, stable=True)[:REQUESTS]
    request_owner = jax.random.permutation(key_mix, seat_owner[taken])
    local_pick = jax.random.randint(key_local, (REQUESTS,), 0, ADP_DEV)
    wanted = request_owner * ADP_DEV + local_pick
    slot_table = jax.random.permutation(key_slot, ADAPTER_POOL).astype(jnp.int32)
    inverse = jnp.argsort(slot_table)
    return (slot_table, inverse[wanted].astype(jnp.int32))


def draw_request_adapter(key, part):
    return placement_draw(key)[1]


def draw_adapter_pool_row(key, part):
    return placement_draw(key)[0]


def touch_ends(array, key, low, top_value):
    longest = array.shape.index(max(array.shape))
    spots = []
    for shift in (0, 1):
        where = [jax.random.randint(jax.random.fold_in(key, axis), (), 0, length) for axis, length in enumerate(array.shape)]
        where[longest] = (where[longest] + shift) % array.shape[longest]
        spots.append(tuple(where))
    return array.at[spots[0]].set(low).at[spots[1]].set(top_value)


def levels(stream_key, dims, shards, smallest, top_value):
    loudness, own = 1.0, jax.random.fold_in(stream_key, 6)
    for position, shards_of in shards:
        heights = jnp.exp(jax.random.uniform(jax.random.fold_in(own, position), (shards_of,), jnp.float32, smallest / len(shards), top_value / len(shards)))
        loudness = loudness * jnp.repeat(heights, dims[position] // shards_of).reshape([-1 if axis == position else 1 for axis in range(len(dims))])
    return loudness


def bell_draw(own_key, extent, scale, bound, cuts=(), kind=jnp.bfloat16):
    array = jax.random.normal(own_key, extent, jnp.float32) * scale
    if len(cuts) > 0:
        array = levels(own_key, extent, cuts, -0.22, 0.18) * array
    return jnp.clip(array, min=-bound, max=bound).astype(kind)


def setup_inputs(seed: int = 0, part: int = 0) -> dict:
    streams_of = jax.random.split(jax.random.key(seed), 13)
    part_keys = jax.random.split(jax.random.fold_in(streams_of[12], part), 13)
    tokens = draw_tokens(jax.random.fold_in(jax.random.fold_in(streams_of[12], part), 71), part)
    query_weight = bell_draw(streams_of[1], (MODEL_WIDTH, QUERY_HEADS * HEAD_SIZE), MODEL_WIDTH ** -0.5, 0.0625, ((1, 2),))
    key_value_weight = bell_draw(streams_of[2], (MODEL_WIDTH, 2 * HEAD_SIZE), MODEL_WIDTH ** -0.5, 0.0625, ((1, 2),))
    output_weight = bell_draw(streams_of[3], (QUERY_HEADS * HEAD_SIZE, MODEL_WIDTH), (QUERY_HEADS * HEAD_SIZE) ** -0.5, 0.25, ((0, 2),))
    adapter_down_maps = bell_draw(part_keys[4], (ADAPTER_POOL, 3 * ADAPTER_RANK, MODEL_WIDTH), MODEL_WIDTH ** -0.5, 0.0625, ((0, 8), (2, 2)))
    adapter_query_up = bell_draw(part_keys[5], (ADAPTER_POOL, ADAPTER_RANK, QUERY_HEADS * HEAD_SIZE), ADAPTER_RANK ** -0.5, 1.5, ((0, 8), (2, 2)))
    adapter_key_value_up = bell_draw(part_keys[6], (ADAPTER_POOL, ADAPTER_RANK, 2 * HEAD_SIZE), ADAPTER_RANK ** -0.5, 1.5, ((0, 8), (2, 2)))
    adapter_output_down = bell_draw(part_keys[7], (ADAPTER_POOL, ADAPTER_RANK, QUERY_HEADS * HEAD_SIZE), (QUERY_HEADS * HEAD_SIZE) ** -0.5, 0.25, ((0, 8), (2, 2)))
    adapter_output_up = bell_draw(part_keys[8], (ADAPTER_POOL, ADAPTER_RANK, MODEL_WIDTH), ADAPTER_RANK ** -0.5, 1.5, ((0, 8), (2, 2)))
    request_adapter = draw_request_adapter(jax.random.fold_in(jax.random.fold_in(streams_of[12], part), 71), part)
    adapter_pool_row = draw_adapter_pool_row(jax.random.fold_in(jax.random.fold_in(streams_of[12], part), 71), part)
    lengths = touch_ends(jax.random.randint(part_keys[11], (REQUESTS,), LEN // 8, LEN + 1), jax.random.fold_in(part_keys[11], 1), LEN // 8, LEN).astype(jnp.int32)
    return {"tokens": tokens, "query_weight": query_weight, "key_value_weight": key_value_weight, "output_weight": output_weight, "adapter_down_maps": adapter_down_maps, "adapter_query_up": adapter_query_up, "adapter_key_value_up": adapter_key_value_up, "adapter_output_down": adapter_output_down, "adapter_output_up": adapter_output_up, "request_adapter": request_adapter, "adapter_pool_row": adapter_pool_row, "lengths": lengths}


def rotate(vectors):
    rows_count, width = vectors.shape
    half_width = width // 2
    freqs = 500000.0 ** (-(jnp.arange(half_width, dtype=jnp.float32) * 2.0 / width))
    angles = jnp.arange(rows_count, dtype=jnp.float32)[:, None] * freqs[None, :]
    cosine = jnp.cos(angles)
    sine_part = jnp.sin(angles)
    first = vectors[:, :half_width]
    second = vectors[:, half_width:]
    return jnp.concatenate([first * cosine - second * sine_part, second * cosine + first * sine_part], axis=1)


def attend(query_rows, key_rows, value_rows, length):
    rows_count = query_rows.shape[0]
    scores = jnp.dot(query_rows, key_rows.T, preferred_element_type=jnp.float32) * (query_rows.shape[1] ** -0.5)
    positions = jnp.arange(rows_count)
    allowed = (positions[None, :] <= positions[:, None]) & (positions[None, :] < length)
    scores = jnp.where(allowed, scores, -1e30)
    highest = jnp.max(scores, axis=1, keepdims=True)
    expo = jnp.exp(scores - highest)
    weights = (expo / jnp.sum(expo, axis=1, keepdims=True)).astype(jnp.bfloat16)
    return jnp.dot(weights, value_rows, preferred_element_type=jnp.float32).astype(jnp.bfloat16)


def reference(tokens, query_weight, key_value_weight, output_weight, adapter_down_maps, adapter_query_up, adapter_key_value_up, adapter_output_down, adapter_output_up, request_adapter, adapter_pool_row, lengths):
    heads = query_weight.shape[1] // HEAD_SIZE
    half_cols = heads * HEAD_SIZE // 2

    def one_request(request):
        x_rows = lax.dynamic_slice_in_dim(tokens, request * LEN, LEN, 0)
        pool_slot = adapter_pool_row[request_adapter[request]]
        down_map_rows = adapter_down_maps[pool_slot]
        query_up_map = adapter_query_up[pool_slot]
        key_value_up = adapter_key_value_up[pool_slot]
        output_down = adapter_output_down[pool_slot]
        output_up = adapter_output_up[pool_slot]
        length = lengths[request]
        shrink = jnp.dot(x_rows, down_map_rows.T, preferred_element_type=jnp.float32).astype(jnp.bfloat16)
        query_all = jnp.dot(x_rows, query_weight, preferred_element_type=jnp.float32) + jnp.dot(shrink[:, :ADAPTER_RANK], query_up_map, preferred_element_type=jnp.float32)
        key_part = jnp.dot(x_rows, key_value_weight[:, :HEAD_SIZE], preferred_element_type=jnp.float32) + jnp.dot(shrink[:, ADAPTER_RANK:2 * ADAPTER_RANK], key_value_up[:, :HEAD_SIZE], preferred_element_type=jnp.float32)
        value_part = jnp.dot(x_rows, key_value_weight[:, HEAD_SIZE:], preferred_element_type=jnp.float32) + jnp.dot(shrink[:, 2 * ADAPTER_RANK:3 * ADAPTER_RANK], key_value_up[:, HEAD_SIZE:], preferred_element_type=jnp.float32)
        key_rounded = lax.optimization_barrier(key_part.astype(jnp.bfloat16))
        key_rows = rotate(key_rounded.astype(jnp.float32)).astype(jnp.bfloat16)
        value_rows = value_part.astype(jnp.bfloat16)
        attended_list = []
        for head in range(heads):
            query_rows = rotate(query_all[:, head * HEAD_SIZE:(head + 1) * HEAD_SIZE]).astype(jnp.bfloat16)
            attended_list.append(attend(query_rows, key_rows, value_rows, length))
        attended_all = jnp.concatenate(attended_list, axis=1)
        base_total = jnp.zeros((LEN, MODEL_WIDTH), jnp.float32)
        for half in range(2):
            term = jnp.dot(attended_all[:, half * half_cols:(half + 1) * half_cols], output_weight[half * half_cols:(half + 1) * half_cols], preferred_element_type=jnp.float32)
            term = lax.optimization_barrier(term.astype(jnp.bfloat16))
            base_total = base_total + term.astype(jnp.float32)
        low = jnp.dot(attended_all, output_down.T, preferred_element_type=jnp.float32).astype(jnp.bfloat16)
        delta_out = jnp.dot(low, output_up, preferred_element_type=jnp.float32)
        valid_rows = (jnp.arange(LEN) < length)[:, None]
        return jnp.where(valid_rows, base_total + delta_out, 0.0).astype(jnp.bfloat16)

    results = lax.map(one_request, jnp.arange(REQUESTS, dtype=jnp.int32))
    return results.reshape(TOKENS, MODEL_WIDTH)
```

```python
import functools

import jax
import jax.numpy as jnp
import numpy as np
from jax import lax
from jax.experimental import pallas as pl
from jax.experimental.pallas import tpu as pltpu
from jax.sharding import PartitionSpec as P

HEAD_SIZE = 128
DOWN_PIECES = 8
UP_PIECES = 2
AHEAD = 2
MESH = pl.DeviceIdType.MESH


def bits_of(size):
    bits = []
    while 2 ** len(bits) < size:
        bits.append(2 ** len(bits))
    return bits[1::-1] + bits[2:]


def subsets(bits):
    masks = [0]
    for bit in bits:
        masks = masks + [mask | bit for mask in masks]
    return masks


def rotary_tables(rows, width):
    half = width // 2
    freqs = np.float32(500000.0) ** (-(np.arange(half, dtype=np.float32) * np.float32(2.0) / np.float32(width)))
    angles = np.arange(rows, dtype=np.float32)[:, None] * freqs.astype(np.float32)[None, :]
    cosine, sine = np.cos(angles), np.sin(angles)
    return np.stack(
        [np.concatenate([cosine, cosine], 1), np.concatenate([-sine, sine], 1)]
    ).astype(np.float32)


def bit_set(number, bit):
    return lax.rem(lax.div(number, bit), 2) == 1


def flip(number, bit):
    return number + bit * (1 - 2 * lax.rem(lax.div(number, bit), 2))


def flip_all(number, mask):
    bit = 1
    while bit <= mask:
        if mask & bit:
            number = flip(number, bit)
        bit *= 2
    return number


def kernel(plan, *refs):
    names = plan["names"]
    r = dict(zip(names, refs))
    size, count, rank = plan["size"], plan["count"], plan["rank"]
    width, q_here, kv_here = plan["width"], plan["q_here"], plan["kv_here"]
    bits, pieces = plan["bits"], plan["pieces"]
    depth = len(bits)
    group = lax.axis_index("group")
    me = lax.axis_index("serve")
    side = lax.axis_index("tensor")
    partner = (group, me, 1 - side)
    neighbours = [(group, flip(me, bit), side) for bit in bits]

    def load(index, src, dst):
        return pltpu.make_async_copy(src, dst, r["load_sem"].at[index])

    own_q = pl.ds(pl.multiple_of(side * q_here, q_here), q_here)
    own_kv = pl.ds(pl.multiple_of(side * kv_here, kv_here), kv_here)
    own_cols = pl.ds(pl.multiple_of(side * width, width), width)
    other_cols = pl.ds(pl.multiple_of((1 - side) * width, width), width)
    loads = [
        load(0, r["adm"], r["down_own"]),
        load(1, r["aqu"], r["small_own"].at[:, :, :q_here]),
        load(2, r["akv"], r["small_own"].at[:, :, q_here : q_here + kv_here]),
        load(3, r["aod"], r["small_own"].at[:, :, q_here + kv_here :]),
        load(4, r["aou"], r["up_own"]),
        load(5, r["tokens"], r["x"].at[side]),
        load(6, r["qw"], r["wq"].at[:, own_q]),
        load(7, r["kvw"], r["wkv"].at[:, own_kv]),
        load(8, r["ow"].at[:, own_cols], r["wo"].at[side]),
        load(9, r["rope"], r["rope_v"]),
    ]
    for copy in loads:
        copy.start()

    barrier = pltpu.get_barrier_semaphore()
    for device in neighbours + [partner]:
        pl.semaphore_signal(barrier, inc=1, device_id=device, device_id_type=MESH)
    pl.semaphore_wait(barrier, len(neighbours) + 1)

    def remote(src, dst, send_sem, recv_sem, device):
        return pltpu.make_async_remote_copy(
            src_ref=src, dst_ref=dst, send_sem=send_sem, recv_sem=recv_sem,
            device_id=device, device_id_type=MESH,
        )

    def stage_copy(stage, index):
        family, start, span = pieces[index]
        cols = slice(start, start + span)
        if stage == 0:
            src, dst = r[family + "_own"], r[family + "_near"]
        else:
            src, dst = r[f"{family}_send{stage}"], r[f"{family}_recv{stage}"]
        return remote(
            src.at[:, :, cols], dst.at[:, :, cols],
            r["hop_send"].at[stage, index], r["hop_recv"].at[stage, index],
            neighbours[stage],
        )

    pair = lambda index, src, dst: remote(
        src, dst, r["pair_send"].at[index], r["pair_recv"].at[index], partner
    )
    pair_tokens = pair(0, r["tokens"], r["x"].at[side])
    pair_q = pair(1, r["qw"], r["wq"].at[:, own_q])
    pair_kv = pair(2, r["kvw"], r["wkv"].at[:, own_kv])
    pair_wo = pair(3, r["ow"].at[:, other_cols], r["wo"].at[side])
    pair_small = pair(4, r["small_all"].at[side], r["small_all"].at[side])
    pair_shrink = pair(5, r["shrink_own"], r["shrink_other"])

    facts = {}
    for mask in subsets(bits):
        wanted = r["pool"][r["req"][flip_all(me, mask)]]
        owner = lax.div(wanted, count)
        facts[mask] = (
            wanted - owner * count,
            [bit_set(owner, bit) != bit_set(me, bit) for bit in bits],
        )

    def chosen(index, mask, stages):
        family, start, span = pieces[index]
        cols = slice(start, start + span)
        slot, differs = facts[mask]

        def of_slot(ref):
            value = ref[0, :, cols]
            for other in range(1, count):
                value = lax.select(slot == other, ref[other, :, cols], value)
            return value

        value = lax.select(differs[0], of_slot(r[family + "_near"]), of_slot(r[family + "_own"]))
        for stage in range(1, stages):
            block = subsets(bits[stage + 1 :]).index(mask)
            arrived = r[f"{family}_recv{stage}"][block, :, cols]
            value = lax.select(differs[stage], arrived, value)
        return value

    def send_stage(stage, index):
        family, start, span = pieces[index]
        cols = slice(start, start + span)
        stage_copy(stage - 1, index).wait_recv()
        for block, mask in enumerate(subsets(bits[stage + 1 :])):
            r[f"{family}_send{stage}"][block, :, cols] = chosen(index, mask | bits[stage], stage)
        stage_copy(stage, index).start()

    own_loaded = {"down": (0,), "small": (1, 2, 3), "up": (4,)}
    loaded = set()

    def need_own(family):
        for index in own_loaded[family]:
            if index not in loaded:
                loads[index].wait()
                loaded.add(index)

    def start_first(index):
        need_own(pieces[index][0])
        stage_copy(0, index).start()

    for index in range(AHEAD):
        start_first(index)
    for copy in (pair_tokens, pair_kv, pair_q, pair_wo):
        copy.start()

    contract = lambda a, b: lax.dot_general(
        a, b, (((1,), (1,)), ((), ())), preferred_element_type=jnp.float32
    )
    mul = lambda a, b: jnp.dot(a, b, preferred_element_type=jnp.float32)

    r["qacc"][...] = jnp.zeros_like(r["qacc"])
    r["kvacc"][...] = jnp.zeros_like(r["kvacc"])
    r["shrink_own"][...] = jnp.zeros_like(r["shrink_own"])
    r["up_maps"][...] = jnp.zeros_like(r["up_maps"])
    three = 3 * rank

    def base_block(number):
        tile = width // DOWN_PIECES
        for half in range(2):
            cols = pl.ds(pl.multiple_of(number * tile, tile), tile)
            rows = pl.ds(pl.multiple_of(half * width + number * tile, tile), tile)
            x_block = r["x"][half, :, cols]
            r["qacc"][...] += mul(x_block, r["wq"][rows, :])
            r["kvacc"][...] += mul(x_block, r["wkv"][rows, :])

    def finish(index):
        family, start, span = pieces[index]
        cols = slice(start, start + span)
        stage_copy(depth - 1, index).wait_recv()
        value = chosen(index, 0, depth)
        if family == "down":
            r["shrink_own"][:, :three] += contract(r["x"][side, :, cols], value)
        elif family == "small":
            r["small_all"][side] = value
            pair_small.start()
        else:
            r["up_all"][:, cols] = value

    n = len(pieces)
    last_down = max(i for i, p in enumerate(pieces) if p[0] == "down")
    first_base = n - 6
    base_done = 0

    def step(number, stages):
        if number + AHEAD < n:
            start_first(number + AHEAD)
        for stage in stages:
            index = number - (stage - 1)
            if 0 <= index < n:
                if stage < depth:
                    send_stage(stage, index)
                else:
                    finish(index)

    all_stages = range(1, depth + 1)
    x_ready = False
    for number in range(last_down + depth):
        if number == depth - 1:
            loads[5].wait()
        step(number, all_stages)
        if number == first_base:
            for index in (6, 7):
                loads[index].wait()
            for copy in (pair_tokens, pair_kv, pair_q):
                copy.wait_recv()
        if number >= first_base and base_done < DOWN_PIECES:
            upto = min(DOWN_PIECES, base_done + 2)

            @pl.loop(base_done, upto)
            def _(block):
                base_block(block)

            base_done = upto
    pair_shrink.start()

    pair_small.wait_recv()
    for half in range(2):
        small = r["small_all"][half]
        r["up_maps"][:rank, half * q_here : (half + 1) * q_here] = small[:, :q_here]
        at = 2 * q_here + half * kv_here
        r["up_maps"][(half + 1) * rank : (half + 2) * rank, at : at + kv_here] = small[
            :, q_here : q_here + kv_here
        ]
        r["out_down"][:, half * q_here : (half + 1) * q_here] = small[:, q_here + kv_here :]
    loads[8].wait()
    loads[9].wait()
    pair_wo.wait_recv()
    pair_shrink.wait_recv()

    shrink = (r["shrink_own"][:, :three] + r["shrink_other"][:, :three]).astype(jnp.bfloat16)
    added = mul(shrink, r["up_maps"][...])
    rows_here = shrink.shape[0]
    kv = (r["kvacc"][...] + added[:, 2 * q_here :]).astype(jnp.bfloat16)
    cos_part, sin_part = r["rope_v"][0], r["rope_v"][1]

    def rotate(v):
        return (v * cos_part + pltpu.roll(v, HEAD_SIZE // 2, 1) * sin_part).astype(jnp.bfloat16)

    keys = rotate(kv[:, :HEAD_SIZE].astype(jnp.float32))
    values = kv[:, HEAD_SIZE:]
    heads = 2 * q_here // HEAD_SIZE
    length = r["lengths"][0]
    line = lax.broadcasted_iota(jnp.int32, (rows_here, rows_here), 0)
    column = lax.broadcasted_iota(jnp.int32, (rows_here, rows_here), 1)
    allowed = (column <= line) & (column < length)
    for head in range(heads):
        at = slice(head * HEAD_SIZE, (head + 1) * HEAD_SIZE)
        query = rotate(r["qacc"][:, at] + added[:, at])
        scores = contract(query, keys) * HEAD_SIZE ** (-0.5)
        scores = jnp.where(allowed, scores, -1e30)
        highest = jnp.max(scores, axis=1, keepdims=True)
        expo = jnp.exp(scores - highest)
        weights = (expo / jnp.sum(expo, axis=1, keepdims=True)).astype(jnp.bfloat16)
        r["attended"][:, at] = mul(weights, values).astype(jnp.bfloat16)
    for number in range(last_down + depth, n + depth - 1):
        step(number, range(1, depth))
    low = contract(r["attended"][...], r["out_down"][...]).astype(jnp.bfloat16)
    for index in range(last_down + 1, n):
        finish(index)
    valid = lax.broadcasted_iota(jnp.int32, (rows_here, 1), 0) < length
    tile = min(512, width)

    @pl.loop(0, width // tile)
    def _(block):
        cols = pl.ds(pl.multiple_of(block * tile, tile), tile)
        total = mul(low, r["up_all"][:, cols])
        base = jnp.zeros((rows_here, tile), jnp.float32)
        for half in range(2):
            term = mul(r["attended"][:, half * q_here : (half + 1) * q_here], r["wo"][half, :, cols])
            base = base + term.astype(jnp.bfloat16).astype(jnp.float32)
        r["out"][:, cols] = jnp.where(valid, base + total, 0.0).astype(jnp.bfloat16)

    for index in range(n):
        for stage in range(depth):
            stage_copy(stage, index).wait_send()
    for copy in (pair_tokens, pair_q, pair_kv, pair_wo, pair_small, pair_shrink):
        copy.wait_send()


def local(tokens, qw, kvw, ow, adm, aqu, akv, aod, aou, req, pool, lengths):
    size = lax.axis_size("serve")
    count, rank, out_width = aou.shape
    rows, width = tokens.shape
    q_here, kv_here = qw.shape[1], kvw.shape[1]
    bits = bits_of(size)
    small_width = q_here + kv_here + q_here
    down_span, up_span = width // DOWN_PIECES, out_width // UP_PIECES
    pieces = [("down", i * down_span, down_span) for i in range(DOWN_PIECES)]
    pieces.insert(1, ("small", 0, small_width))
    pieces += [("up", i * up_span, up_span) for i in range(UP_PIECES)]
    shapes = {
        "down": (adm.shape[1], width),
        "small": (rank, small_width),
        "up": (rank, out_width),
    }
    bf16, f32 = jnp.bfloat16, jnp.float32
    scratch = {}
    for family, (lines, span) in shapes.items():
        scratch[family + "_own"] = pltpu.VMEM((count, lines, span), bf16)
        scratch[family + "_near"] = pltpu.VMEM((count, lines, span), bf16)
        for stage in range(1, len(bits)):
            blocks = 2 ** (len(bits) - 1 - stage)
            scratch[f"{family}_send{stage}"] = pltpu.VMEM((blocks, lines, span), bf16)
            scratch[f"{family}_recv{stage}"] = pltpu.VMEM((blocks, lines, span), bf16)
    scratch.update(
        small_all=pltpu.VMEM((2, rank, small_width), bf16),
        up_all=pltpu.VMEM((rank, out_width), bf16),
        x=pltpu.VMEM((2, rows, width), bf16),
        wq=pltpu.VMEM((qw.shape[0], 2 * q_here), bf16),
        wkv=pltpu.VMEM((kvw.shape[0], 2 * kv_here), bf16),
        wo=pltpu.VMEM((2, ow.shape[0], out_width), bf16),
        rope_v=pltpu.VMEM((2, rows, HEAD_SIZE), f32),
        qacc=pltpu.VMEM((rows, 2 * q_here), f32),
        kvacc=pltpu.VMEM((rows, 2 * kv_here), f32),
        shrink_own=pltpu.VMEM((rows, 128), f32),
        shrink_other=pltpu.VMEM((rows, 128), f32),
        up_maps=pltpu.VMEM((3 * rank, 2 * q_here + 2 * kv_here), bf16),
        out_down=pltpu.VMEM((rank, 2 * q_here), bf16),
        attended=pltpu.VMEM((rows, 2 * q_here), bf16),
        load_sem=pltpu.SemaphoreType.DMA((10,)),
        hop_send=pltpu.SemaphoreType.DMA((len(bits), len(pieces))),
        hop_recv=pltpu.SemaphoreType.DMA((len(bits), len(pieces))),
        pair_send=pltpu.SemaphoreType.DMA((6,)),
        pair_recv=pltpu.SemaphoreType.DMA((6,)),
    )
    operands = ["req", "pool", "lengths", "tokens", "qw", "kvw", "ow", "adm", "aqu", "akv", "aod", "aou", "rope"]
    plan = dict(
        names=operands + ["out"] + list(scratch),
        size=size, count=count, rank=rank, width=width, q_here=q_here, kv_here=kv_here,
        bits=bits, pieces=pieces,
    )
    rope = jnp.asarray(rotary_tables(rows, HEAD_SIZE))
    smem = pl.BlockSpec(memory_space=pltpu.SMEM)
    hbm = pl.BlockSpec(memory_space=pl.ANY)
    return pl.pallas_call(
        functools.partial(kernel, plan),
        out_shape=jax.ShapeDtypeStruct((rows, out_width), bf16),
        in_specs=[smem] * 3 + [hbm] * 10,
        out_specs=pl.BlockSpec(memory_space=pltpu.VMEM),
        scratch_shapes=list(scratch.values()),
        compiler_params=pltpu.CompilerParams(
            collective_id=0, has_side_effects=True, vmem_limit_bytes=60 * 1024 * 1024
        ),
        name="routed_attention",
    )(req, pool, lengths, tokens, qw, kvw, ow, adm, aqu, akv, aod, aou, rope)


def solution(mesh):
    placed = (
        P(("group", "serve"), "tensor"),
        P(None, "tensor"),
        P(None, "tensor"),
        P("tensor", None),
        P(("group", "serve"), None, "tensor"),
        P(("group", "serve"), None, "tensor"),
        P(("group", "serve"), None, "tensor"),
        P(("group", "serve"), None, "tensor"),
        P(("group", "serve"), None, "tensor"),
        P("group"),
        P("group"),
        P(("group", "serve")),
    )
    return jax.shard_map(
        local,
        mesh=mesh,
        in_specs=placed,
        out_specs=P(("group", "serve"), "tensor"),
        check_vma=False,
    )
```

```python
import functools

import jax
import jax.numpy as jnp
import numpy as np
from jax import lax
from jax.experimental import pallas as pl
from jax.experimental.pallas import tpu as pltpu
from jax.sharding import PartitionSpec as P

HEAD_SIZE = 128
DOWN_PIECES = 8
UP_PIECES = 2
BASE_PIECES = 8
AHEAD = 2
LAG_C = 1
LAG_D = 3
LAG_F = 2
MESH = pl.DeviceIdType.MESH


def rotary_tables(rows, width):
    half = width // 2
    freqs = np.float32(500000.0) ** (-(np.arange(half, dtype=np.float32) * np.float32(2.0) / np.float32(width)))
    angles = np.arange(rows, dtype=np.float32)[:, None] * freqs.astype(np.float32)[None, :]
    cosine, sine = np.cos(angles), np.sin(angles)
    return np.stack(
        [np.concatenate([cosine, cosine], 1), np.concatenate([-sine, sine], 1)]
    ).astype(np.float32)


def hub_of(pair, levels):
    return 2 * pair + 1 if 2 * pair + 1 < levels // 2 else 2 * pair


def kernel(plan, *refs):
    r = dict(zip(plan["names"], refs))
    count, rank, levels = plan["count"], plan["rank"], plan["levels"]
    width, q_here, kv_here = plan["width"], plan["q_here"], plan["kv_here"]
    pieces = plan["pieces"]
    n = len(pieces)
    pairs = levels // 2
    group = lax.axis_index("group")
    me = lax.axis_index("serve")
    side = lax.axis_index("tensor")
    level = lax.div(me, 2)
    col = lax.rem(me, 2)
    pair = lax.div(level, 2)
    upper = jnp.where(2 * pair + 1 < pairs, 0, 1)
    is_hub = lax.rem(level, 2) != upper
    is_end = lax.rem(level, 2) == upper
    mate = level + 1 - 2 * lax.rem(level, 2)
    core_mate = (group, me, 1 - side)
    col_mate = (group, level * 2 + 1 - col, side)
    level_mate = (group, mate * 2 + col, side)

    def load(index, src, dst):
        return pltpu.make_async_copy(src, dst, r["load_sem"].at[index])

    own_q = pl.ds(pl.multiple_of(side * q_here, q_here), q_here)
    own_kv = pl.ds(pl.multiple_of(side * kv_here, kv_here), kv_here)
    own_cols = pl.ds(pl.multiple_of(side * width, width), width)
    other_cols = pl.ds(pl.multiple_of((1 - side) * width, width), width)
    loads = [
        load(0, r["tokens"], r["x"].at[side]),
        load(1, r["qw"], r["wq"].at[:, own_q]),
        load(2, r["kvw"], r["wkv"].at[:, own_kv]),
        load(3, r["ow"].at[:, own_cols], r["wo"].at[side]),
        load(4, r["rope"], r["rope_v"]),
    ]
    load_tokens, load_q, load_kv, load_wo, load_rope = loads
    raw = [r[f"raw{index}"] for index in range(n)]
    give = [r[f"give{index}"] for index in range(n)]
    sends = [r[f"sends{index}"] for index in range(n)]
    hubs = [r[f"hubs{index}"] for index in range(n)]
    on = [r[f"on{index}"] for index in range(n)]
    got = [r[f"got{index}"] for index in range(n)]
    spans = [ref.shape[-1] for ref in got]
    piece_loads = []
    for index, (family, number) in enumerate(pieces):
        copies = []
        for slot, half, dst in ((0, col, raw[index].at[pl.ds(0, count)]), (1, 1 - col, give[index])):
            if family == "small":
                lines = pl.ds(pl.multiple_of(half * (rank // 2), rank // 2), rank // 2)
                at = 0
                for part, name in enumerate(("aqu", "akv", "aod")):
                    wide = r[name].shape[-1]
                    sem = len(loads) + 2 * n + 2 * part + slot
                    copies.append(load(sem, r[name].at[:, lines, :], dst.at[:, :, at : at + wide]))
                    at += wide
            else:
                src = r["adm" if family == "down" else "aou"]
                span = spans[index]
                at = pl.ds(pl.multiple_of((2 * number + half) * span, span), span)
                copies.append(load(len(loads) + 2 * index + slot, src.at[:, :, at], dst))
        piece_loads.append(copies)
    for copies in piece_loads:
        for copy in copies:
            copy.start()
    for copy in loads:
        copy.start()

    barrier = pltpu.get_barrier_semaphore()

    def greet(device):
        pl.semaphore_signal(barrier, inc=1, device_id=device, device_id_type=MESH)

    greet(core_mate)
    greet(col_mate)
    for other in range(levels):
        other_hub = other == hub_of(other // 2, levels)

        @pl.when((level != other) if other_hub else ((level != other) & is_hub))
        def _():
            greet((group, other * 2 + col, side))

    pl.semaphore_wait(barrier, jnp.where(is_hub, levels + 1, pairs + 2))

    def remote(src, dst, send_sem, recv_sem, device):
        return pltpu.make_async_remote_copy(
            src_ref=src, dst_ref=dst, send_sem=send_sem, recv_sem=recv_sem,
            device_id=device, device_id_type=MESH,
        )

    def hop(kind, index, src, dst, device):
        return remote(src, dst, r["hop_send"].at[kind, index], r["hop_recv"].at[kind, index], device)

    def raws(index, at):
        return raw[index].at[pl.ds(at * count, count)]

    def copy_a(index):
        return hop(0, index, give[index], raws(index, 1), col_mate)

    def copy_b_own(index):
        return hop(1, index, raws(index, 0), raws(index, 2), level_mate)

    def copy_b_relay(index):
        return hop(2, index, raws(index, 1), raws(index, 3), level_mate)

    def copy_c(index, to, hub_pair):
        return remote(
            sends[index].at[to],
            hubs[index].at[hub_pair],
            r["c_send"].at[index, to],
            r["c_recv"].at[index, hub_pair],
            (group, to * 2 + col, side),
        )

    def copy_d(index):
        family, number = pieces[index]
        dst = {
            "down": lambda: got[index],
            "small": lambda: r["small_all"].at[side, col],
            "up": lambda: r["up_all"].at[number, col],
        }[family]()
        return hop(3, index, on[index], dst, col_mate)

    pair_copy = lambda index, src, dst: remote(
        src, dst, r["pair_send"].at[index], r["pair_recv"].at[index], core_mate
    )
    pair_tokens = pair_copy(0, r["tokens"], r["x"].at[side])
    pair_q = pair_copy(1, r["qw"], r["wq"].at[:, own_q])
    pair_kv = pair_copy(2, r["kvw"], r["wkv"].at[:, own_kv])
    pair_wo = pair_copy(3, r["ow"].at[:, other_cols], r["wo"].at[side])
    pair_small = pair_copy(4, r["small_all"].at[side], r["small_all"].at[side])
    pair_shrink = pair_copy(5, r["shrink_own"], r["shrink_other"])

    def facts(target):
        wanted = r["pool"][r["req"][target]]
        owner = lax.div(wanted, count)
        owner_level = lax.div(owner, 2)
        away = jnp.where(lax.rem(owner_level, 2) == lax.rem(level, 2), 0, 2)
        aside = jnp.where(lax.rem(owner, 2) == col, 0, 1)
        return (away + aside) * count + wanted - owner * count, lax.div(owner_level, 2)

    own_facts = [facts(level * 2 + col), facts(level * 2 + 1 - col)]
    level_facts = [[facts(to * 2 + col), facts(to * 2 + 1 - col)] for to in range(levels)]

    def cols_of(index, half):
        number, span = pieces[index][1], spans[index]
        return pl.ds(pl.multiple_of((2 * number + half) * span, span), span)

    contract = lambda a, b: lax.dot_general(
        a, b, (((1,), (1,)), ((), ())), preferred_element_type=jnp.float32
    )
    mul = lambda a, b: jnp.dot(a, b, preferred_element_type=jnp.float32)
    three = 3 * rank

    def start(index):
        for copy in piece_loads[index]:
            copy.wait()
        copy_a(index).start()

        @pl.when(is_end)
        def _():
            copy_b_own(index).start()

    def relay(index):
        copy_a(index).wait_recv()

        @pl.when(is_end)
        def _():
            copy_b_relay(index).start()

    def choose(index):
        @pl.when(is_hub)
        def _():
            copy_b_own(index).wait_recv()
            copy_b_relay(index).wait_recv()
            for to in sorted(range(levels), key=lambda z: abs(2 * z + 1 - levels)):

                @pl.when(level != to)
                def _():
                    for block in range(2):
                        sends[index][to, block] = raw[index][level_facts[to][block][0]]
                    copy_c(index, to, pair).start()

            for block in range(2):
                hubs[index][pair, block] = raw[index][own_facts[block][0]]

    def pick(index):
        family, number = pieces[index]
        for hub in range(pairs):

            @pl.when(level != hub_of(hub, levels))
            def _():
                copy_c(index, hub_of(hub, levels), hub).wait_recv()

        on[index][...] = hubs[index][own_facts[1][1], 1]
        copy_d(index).start()
        value = hubs[index][own_facts[0][1], 0]
        if family == "down":
            r["shrink_own"][:, :three] += contract(r["x"][side, :, cols_of(index, col)], value)
        elif family == "small":
            r["small_all"][side, col] = value
        else:
            r["up_all"][number, col] = value

    def finish(index):
        family, number = pieces[index]
        copy_d(index).wait_recv()
        if family == "down":
            r["shrink_own"][:, :three] += contract(
                r["x"][side, :, cols_of(index, 1 - col)], got[index][...]
            )
        elif family == "small":
            pair_small.start()

    for index in range(AHEAD):
        start(index)
    for copy in (pair_tokens, pair_kv, pair_q, pair_wo):
        copy.start()

    r["qacc"][...] = jnp.zeros_like(r["qacc"])
    r["kvacc"][...] = jnp.zeros_like(r["kvacc"])
    r["shrink_own"][...] = jnp.zeros_like(r["shrink_own"])
    r["up_maps"][...] = jnp.zeros_like(r["up_maps"])

    def base_block(number):
        tile = width // BASE_PIECES
        for half in range(2):
            cols = pl.ds(pl.multiple_of(number * tile, tile), tile)
            rows = pl.ds(pl.multiple_of(half * width + number * tile, tile), tile)
            x_block = r["x"][half, :, cols]
            r["qacc"][...] += mul(x_block, r["wq"][rows, :])
            r["kvacc"][...] += mul(x_block, r["wkv"][rows, :])

    last_down = max(i for i, p in enumerate(pieces) if p[0] == "down")
    done = {start: AHEAD, relay: 0, choose: 0, pick: 0, finish: 0}
    lags = {start: -AHEAD, relay: 0, choose: LAG_C, pick: LAG_C + LAG_D, finish: LAG_C + LAG_D + LAG_F}

    def up_to(action, index):
        while done[action] <= min(index, n - 1):
            action(done[action])
            done[action] += 1

    base_done = 0
    steps = last_down + lags[finish] + 1
    first_base = steps - 5
    for number in range(steps):
        for action in (start, relay, choose, pick, finish):
            if action is pick and done[pick] == 0 and number == lags[pick]:
                load_tokens.wait()
            up_to(action, number - lags[action])
        if number == first_base:
            load_q.wait()
            load_kv.wait()
            for copy in (pair_tokens, pair_kv, pair_q):
                copy.wait_recv()
        if number >= first_base and base_done < BASE_PIECES:
            upto = min(BASE_PIECES, base_done + 2)

            @pl.loop(base_done, upto)
            def _(block):
                base_block(block)

            base_done = upto
    pair_shrink.start()

    up_to(relay, n)
    up_to(choose, n)
    pair_small.wait_recv()
    lines = rank // 2
    for half in range(2):
        own = slice(half * q_here, (half + 1) * q_here)
        at = 2 * q_here + half * kv_here
        for part in range(2):
            small = r["small_all"][half, part]
            to = slice(part * lines, (part + 1) * lines)
            r["up_maps"][to, own] = small[:, :q_here]
            to_kv = slice((half + 1) * rank + part * lines, (half + 1) * rank + (part + 1) * lines)
            r["up_maps"][to_kv, at : at + kv_here] = small[:, q_here : q_here + kv_here]
            r["out_down"][to, own] = small[:, q_here + kv_here :]
    load_wo.wait()
    load_rope.wait()
    pair_wo.wait_recv()
    pair_shrink.wait_recv()

    shrink = (r["shrink_own"][:, :three] + r["shrink_other"][:, :three]).astype(jnp.bfloat16)
    added = mul(shrink, r["up_maps"][...])
    rows_here = shrink.shape[0]
    kv = (r["kvacc"][...] + added[:, 2 * q_here :]).astype(jnp.bfloat16)
    cos_part, sin_part = r["rope_v"][0], r["rope_v"][1]

    def rotate(v):
        return (v * cos_part + pltpu.roll(v, HEAD_SIZE // 2, 1) * sin_part).astype(jnp.bfloat16)

    keys = rotate(kv[:, :HEAD_SIZE].astype(jnp.float32))
    values = kv[:, HEAD_SIZE:]
    heads = 2 * q_here // HEAD_SIZE
    length = r["lengths"][0]
    line = lax.broadcasted_iota(jnp.int32, (rows_here, rows_here), 0)
    column = lax.broadcasted_iota(jnp.int32, (rows_here, rows_here), 1)
    allowed = (column <= line) & (column < length)
    for head in range(heads):
        at = slice(head * HEAD_SIZE, (head + 1) * HEAD_SIZE)
        query = rotate(r["qacc"][:, at] + added[:, at])
        scores = contract(query, keys) * HEAD_SIZE ** (-0.5)
        scores = jnp.where(allowed, scores, -1e30)
        highest = jnp.max(scores, axis=1, keepdims=True)
        expo = jnp.exp(scores - highest)
        weights = (expo / jnp.sum(expo, axis=1, keepdims=True)).astype(jnp.bfloat16)
        r["attended"][:, at] = mul(weights, values).astype(jnp.bfloat16)
    up_to(pick, n)
    low = contract(r["attended"][...], r["out_down"][...]).astype(jnp.bfloat16)
    up_to(finish, n)
    valid = lax.broadcasted_iota(jnp.int32, (rows_here, 1), 0) < length
    up_span = r["up_all"].shape[-1]
    tile = min(512, up_span)
    per = up_span // tile

    @pl.loop(0, width // tile)
    def _(block):
        cols = pl.ds(pl.multiple_of(block * tile, tile), tile)
        part = lax.div(block, per)
        inner = pl.ds(pl.multiple_of((block - part * per) * tile, tile), tile)
        total = mul(low, r["up_all"][lax.div(part, 2), lax.rem(part, 2), :, inner])
        base = jnp.zeros((rows_here, tile), jnp.float32)
        for half in range(2):
            term = mul(r["attended"][:, half * q_here : (half + 1) * q_here], r["wo"][half, :, cols])
            base = base + term.astype(jnp.bfloat16).astype(jnp.float32)
        r["out"][:, cols] = jnp.where(valid, base + total, 0.0).astype(jnp.bfloat16)

    for index in range(n):
        copy_a(index).wait_send()
        copy_d(index).wait_send()

        @pl.when(is_end)
        def _():
            copy_b_own(index).wait_send()
            copy_b_relay(index).wait_send()

        @pl.when(is_hub)
        def _():
            for to in range(levels):

                @pl.when(level != to)
                def _():
                    copy_c(index, to, pair).wait_send()

    for copy in (pair_tokens, pair_q, pair_kv, pair_wo, pair_small, pair_shrink):
        copy.wait_send()


def local(tokens, qw, kvw, ow, adm, aqu, akv, aod, aou, req, pool, lengths):
    size = lax.axis_size("serve")
    count, rank, out_width = aou.shape
    rows, width = tokens.shape
    q_here, kv_here = qw.shape[1], kvw.shape[1]
    levels = size // 2
    small_width = q_here + kv_here + q_here
    down_span, up_span = width // (2 * DOWN_PIECES), out_width // (2 * UP_PIECES)
    pieces = [("down", i) for i in range(DOWN_PIECES)]
    pieces.insert(1, ("small", 0))
    pieces += [("up", i) for i in range(UP_PIECES)]
    shapes = {
        "down": (adm.shape[1], down_span),
        "small": (rank // 2, small_width),
        "up": (rank, up_span),
    }
    bf16, f32 = jnp.bfloat16, jnp.float32
    scratch = {}
    for index, (family, _) in enumerate(pieces):
        lines, span = shapes[family]
        kinds = {
            "raw": (4 * count,), "give": (count,), "sends": (levels, 2),
            "hubs": (levels // 2, 2), "on": (), "got": (),
        }
        for kind, lead in kinds.items():
            scratch[f"{kind}{index}"] = pltpu.VMEM((*lead, lines, span), bf16)
    scratch.update(
        small_all=pltpu.VMEM((2, 2, rank // 2, small_width), bf16),
        up_all=pltpu.VMEM((UP_PIECES, 2, rank, up_span), bf16),
        x=pltpu.VMEM((2, rows, width), bf16),
        wq=pltpu.VMEM((qw.shape[0], 2 * q_here), bf16),
        wkv=pltpu.VMEM((kvw.shape[0], 2 * kv_here), bf16),
        wo=pltpu.VMEM((2, ow.shape[0], out_width), bf16),
        rope_v=pltpu.VMEM((2, rows, HEAD_SIZE), f32),
        qacc=pltpu.VMEM((rows, 2 * q_here), f32),
        kvacc=pltpu.VMEM((rows, 2 * kv_here), f32),
        shrink_own=pltpu.VMEM((rows, 128), f32),
        shrink_other=pltpu.VMEM((rows, 128), f32),
        up_maps=pltpu.VMEM((3 * rank, 2 * q_here + 2 * kv_here), bf16),
        out_down=pltpu.VMEM((rank, 2 * q_here), bf16),
        attended=pltpu.VMEM((rows, 2 * q_here), bf16),
        load_sem=pltpu.SemaphoreType.DMA((5 + 2 * len(pieces) + 6,)),
        hop_send=pltpu.SemaphoreType.DMA((4, len(pieces))),
        hop_recv=pltpu.SemaphoreType.DMA((4, len(pieces))),
        c_send=pltpu.SemaphoreType.DMA((len(pieces), levels)),
        c_recv=pltpu.SemaphoreType.DMA((len(pieces), levels // 2)),
        pair_send=pltpu.SemaphoreType.DMA((6,)),
        pair_recv=pltpu.SemaphoreType.DMA((6,)),
    )
    operands = ["req", "pool", "lengths", "tokens", "qw", "kvw", "ow", "adm", "aqu", "akv", "aod", "aou", "rope"]
    plan = dict(
        names=operands + ["out"] + list(scratch),
        levels=levels, count=count, rank=rank, width=width, q_here=q_here, kv_here=kv_here,
        pieces=pieces,
    )
    rope = jnp.asarray(rotary_tables(rows, HEAD_SIZE))
    smem = pl.BlockSpec(memory_space=pltpu.SMEM)
    hbm = pl.BlockSpec(memory_space=pl.ANY)
    return pl.pallas_call(
        functools.partial(kernel, plan),
        out_shape=jax.ShapeDtypeStruct((rows, out_width), bf16),
        in_specs=[smem] * 3 + [hbm] * 10,
        out_specs=pl.BlockSpec(memory_space=pltpu.VMEM),
        scratch_shapes=list(scratch.values()),
        compiler_params=pltpu.CompilerParams(
            collective_id=0, has_side_effects=True, vmem_limit_bytes=60 * 1024 * 1024
        ),
        name="routed_attention",
    )(req, pool, lengths, tokens, qw, kvw, ow, adm, aqu, akv, aod, aou, rope)


def solution(mesh):
    placed = (
        P(("group", "serve"), "tensor"),
        P(None, "tensor"),
        P(None, "tensor"),
        P("tensor", None),
        P(("group", "serve"), None, "tensor"),
        P(("group", "serve"), None, "tensor"),
        P(("group", "serve"), None, "tensor"),
        P(("group", "serve"), None, "tensor"),
        P(("group", "serve"), None, "tensor"),
        P("group"),
        P("group"),
        P(("group", "serve")),
    )
    return jax.shard_map(
        local,
        mesh=mesh,
        in_specs=placed,
        out_specs=P(("group", "serve"), "tensor"),
        check_vma=False,
    )
```

```python
import functools

import jax
import jax.numpy as jnp
import numpy as np
from jax import lax
from jax.experimental import pallas as pl
from jax.experimental.pallas import tpu as pltpu
from jax.sharding import PartitionSpec as P

HEAD_SIZE = 128
DOWN_PIECES = 8
UP_PIECES = 2
BASE_PIECES = 8
AHEAD = 2
LAG_C = 1
LAG_P = 3
CHOOSE_1 = 9
MESH = pl.DeviceIdType.MESH


def rotary_tables(rows, width):
    half = width // 2
    freqs = np.float32(500000.0) ** (-(np.arange(half, dtype=np.float32) * np.float32(2.0) / np.float32(width)))
    angles = np.arange(rows, dtype=np.float32)[:, None] * freqs.astype(np.float32)[None, :]
    cosine, sine = np.cos(angles), np.sin(angles)
    return np.stack(
        [np.concatenate([cosine, cosine], 1), np.concatenate([-sine, sine], 1)]
    ).astype(np.float32)


def hub_of(pair, levels):
    return 2 * pair + 1 if 2 * pair + 1 < levels // 2 else 2 * pair


def kernel(plan, *refs):
    r = dict(zip(plan["names"], refs))
    count, rank, levels = plan["count"], plan["rank"], plan["levels"]
    width, q_here, kv_here = plan["width"], plan["q_here"], plan["kv_here"]
    pieces = plan["pieces"]
    n = len(pieces)
    pairs = levels // 2
    group = lax.axis_index("group")
    me = lax.axis_index("serve")
    side = lax.axis_index("tensor")
    level = lax.div(me, 2)
    col = lax.rem(me, 2)
    pair = lax.div(level, 2)
    upper = jnp.where(2 * pair + 1 < pairs, 0, 1)
    is_hub = lax.rem(level, 2) != upper
    is_end = lax.rem(level, 2) == upper
    mate = level + 1 - 2 * lax.rem(level, 2)
    core_mate = (group, me, 1 - side)
    col_mate = (group, level * 2 + 1 - col, side)
    level_mate = (group, mate * 2 + col, side)

    def load(index, src, dst):
        return pltpu.make_async_copy(src, dst, r["load_sem"].at[index])

    own_q = pl.ds(pl.multiple_of(side * q_here, q_here), q_here)
    own_kv = pl.ds(pl.multiple_of(side * kv_here, kv_here), kv_here)
    own_cols = pl.ds(pl.multiple_of(side * width, width), width)
    other_cols = pl.ds(pl.multiple_of((1 - side) * width, width), width)
    loads = [
        load(0, r["tokens"], r["x"].at[side]),
        load(1, r["qw"], r["wq"].at[:, own_q]),
        load(2, r["kvw"], r["wkv"].at[:, own_kv]),
        load(3, r["ow"].at[:, own_cols], r["wo"].at[side]),
        load(4, r["rope"], r["rope_v"]),
    ]
    load_tokens, load_q, load_kv, load_wo, load_rope = loads
    raw = [r[f"raw{index}"] for index in range(n)]
    give = [r[f"give{index}"] for index in range(n)]
    sends = [r[f"sends{index}"] for index in range(n)]
    hubs = [r[f"hubs{index}"] for index in range(n)]
    spans = [ref.shape[-1] for ref in give]
    piece_loads = []
    for index, (family, number) in enumerate(pieces):
        copies = []
        for slot, half, dst in ((0, col, raw[index].at[pl.ds(0, count)]), (1, 1 - col, give[index])):
            if family == "small":
                lines = pl.ds(pl.multiple_of(half * (rank // 2), rank // 2), rank // 2)
                at = 0
                for part, name in enumerate(("aqu", "akv", "aod")):
                    wide = r[name].shape[-1]
                    sem = len(loads) + 2 * n + 2 * part + slot
                    copies.append(load(sem, r[name].at[:, lines, :], dst.at[:, :, at : at + wide]))
                    at += wide
            else:
                src = r["adm" if family == "down" else "aou"]
                span = spans[index]
                at = pl.ds(pl.multiple_of((2 * number + half) * span, span), span)
                copies.append(load(len(loads) + 2 * index + slot, src.at[:, :, at], dst))
        piece_loads.append(copies)
    for copies in piece_loads:
        for copy in copies:
            copy.start()
    for copy in loads:
        copy.start()

    barrier = pltpu.get_barrier_semaphore()

    def greet(device):
        pl.semaphore_signal(barrier, inc=1, device_id=device, device_id_type=MESH)

    greet(core_mate)
    for other in range(2 * levels):
        other_hub = other // 2 == hub_of(other // 4, levels)

        @pl.when((me != other) if other_hub else ((me != other) & is_hub))
        def _():
            greet((group, other, side))

    @pl.when(is_end)
    def _():
        greet(col_mate)

    pl.semaphore_wait(barrier, jnp.where(is_hub, 2 * levels, 2 * pairs + 2))

    def remote(src, dst, send_sem, recv_sem, device):
        return pltpu.make_async_remote_copy(
            src_ref=src, dst_ref=dst, send_sem=send_sem, recv_sem=recv_sem,
            device_id=device, device_id_type=MESH,
        )

    def hop(kind, index, src, dst, device):
        return remote(src, dst, r["hop_send"].at[kind, index], r["hop_recv"].at[kind, index], device)

    def raws(index, at):
        return raw[index].at[pl.ds(at * count, count)]

    def copy_a(index):
        return hop(0, index, give[index], raws(index, 1), col_mate)

    def copy_b_own(index):
        return hop(1, index, raws(index, 0), raws(index, 2), level_mate)

    def copy_b_relay(index):
        return hop(2, index, raws(index, 1), raws(index, 3), level_mate)

    def copy_c(index, half, to, hub_pair):
        return remote(
            sends[index].at[to],
            hubs[index].at[half, hub_pair],
            r["c_send"].at[index, to],
            r["c_recv"].at[index, half, hub_pair],
            (group, to, side),
        )

    pair_copy = lambda index, src, dst: remote(
        src, dst, r["pair_send"].at[index], r["pair_recv"].at[index], core_mate
    )
    pair_tokens = pair_copy(0, r["tokens"], r["x"].at[side])
    pair_q = pair_copy(1, r["qw"], r["wq"].at[:, own_q])
    pair_kv = pair_copy(2, r["kvw"], r["wkv"].at[:, own_kv])
    pair_wo = pair_copy(3, r["ow"].at[:, other_cols], r["wo"].at[side])
    pair_small = pair_copy(4, r["small_all"].at[side], r["small_all"].at[side])
    pair_shrink = pair_copy(5, r["shrink_own"], r["shrink_other"])

    def facts(target):
        wanted = r["pool"][r["req"][target]]
        owner = lax.div(wanted, count)
        owner_level = lax.div(owner, 2)
        away = jnp.where(lax.rem(owner_level, 2) == lax.rem(level, 2), 0, 2)
        aside = jnp.where(lax.rem(owner, 2) == col, 0, 1)
        return (away + aside) * count + wanted - owner * count, lax.div(owner_level, 2)

    mine = facts(me)
    wants = [facts(to) for to in range(2 * levels)]

    contract = lambda a, b: lax.dot_general(
        a, b, (((1,), (1,)), ((), ())), preferred_element_type=jnp.float32
    )
    mul = lambda a, b: jnp.dot(a, b, preferred_element_type=jnp.float32)
    three = 3 * rank

    def start(index):
        for copy in piece_loads[index]:
            copy.wait()
        copy_a(index).start()

        @pl.when(is_end)
        def _():
            copy_b_own(index).start()

    def relay(index):
        copy_a(index).wait_recv()

        @pl.when(is_end)
        def _():
            copy_b_relay(index).start()

    send_order = sorted(range(2 * levels), key=lambda to: -abs(2 * (to // 2) + 1 - levels))

    def choose(index):
        @pl.when(is_hub)
        def _():
            copy_b_own(index).wait_recv()
            copy_b_relay(index).wait_recv()
            for to in send_order:

                @pl.when(me != to)
                def _():
                    sends[index][to] = raw[index][wants[to][0]]
                    copy_c(index, col, to, pair).start()

            hubs[index][col, pair] = raw[index][mine[0]]

    def pick(index):
        family, number = pieces[index]
        for half in range(2):
            for hub in range(pairs):

                @pl.when(me != 2 * hub_of(hub, levels) + half)
                def _():
                    copy_c(index, half, 2 * hub_of(hub, levels) + half, hub).wait_recv()

        for half in range(2):
            value = hubs[index][half, mine[1]]
            if family == "down":
                at = (2 * number + half) * spans[index]
                x_part = r["x"][side, :, at : at + spans[index]]
                r["shrink_own"][:, :three] += contract(x_part, value)
            elif family == "small":
                r["small_all"][side, half] = value
            else:
                r["up_all"][number, half] = value
        if family == "small":
            pair_small.start()

    for index in range(AHEAD):
        start(index)
    for copy in (pair_tokens, pair_kv, pair_q, pair_wo):
        copy.start()

    r["qacc"][...] = jnp.zeros_like(r["qacc"])
    r["kvacc"][...] = jnp.zeros_like(r["kvacc"])
    r["shrink_own"][...] = jnp.zeros_like(r["shrink_own"])
    r["up_maps"][...] = jnp.zeros_like(r["up_maps"])

    def base_block(number):
        tile = width // BASE_PIECES
        for half in range(2):
            cols = pl.ds(pl.multiple_of(number * tile, tile), tile)
            rows = pl.ds(pl.multiple_of(half * width + number * tile, tile), tile)
            x_block = r["x"][half, :, cols]
            r["qacc"][...] += mul(x_block, r["wq"][rows, :])
            r["kvacc"][...] += mul(x_block, r["wkv"][rows, :])

    last_down = max(i for i, p in enumerate(pieces) if p[0] == "down")
    done = {start: AHEAD, relay: 0, choose: 0, pick: 0}
    lags = {start: -AHEAD, relay: 0, choose: LAG_C, pick: LAG_C + LAG_P}

    def up_to(action, index):
        while done[action] <= min(index, n - 1):
            action(done[action])
            done[action] += 1

    base_done = 0
    steps = last_down + lags[pick] + 1
    first_base = steps - 5
    for number in range(steps):
        for action in (start, relay, choose, pick):
            if action is pick and done[pick] == 0 and number == lags[pick]:
                load_tokens.wait()
            up_to(action, number - lags[action])
        if number == first_base:
            load_q.wait()
            load_kv.wait()
            for copy in (pair_tokens, pair_kv, pair_q):
                copy.wait_recv()
        if number >= first_base and base_done < BASE_PIECES:
            upto = min(BASE_PIECES, base_done + 2)

            @pl.loop(base_done, upto)
            def _(block):
                base_block(block)

            base_done = upto
    pair_shrink.start()

    up_to(relay, n)
    up_to(choose, CHOOSE_1)
    pair_small.wait_recv()
    lines = rank // 2
    for half in range(2):
        own = slice(half * q_here, (half + 1) * q_here)
        at = 2 * q_here + half * kv_here
        for part in range(2):
            small = r["small_all"][half, part]
            to = slice(part * lines, (part + 1) * lines)
            r["up_maps"][to, own] = small[:, :q_here]
            to_kv = slice((half + 1) * rank + part * lines, (half + 1) * rank + (part + 1) * lines)
            r["up_maps"][to_kv, at : at + kv_here] = small[:, q_here : q_here + kv_here]
            r["out_down"][to, own] = small[:, q_here + kv_here :]
    load_wo.wait()
    load_rope.wait()
    pair_wo.wait_recv()
    pair_shrink.wait_recv()

    shrink = (r["shrink_own"][:, :three] + r["shrink_other"][:, :three]).astype(jnp.bfloat16)
    added = mul(shrink, r["up_maps"][...])
    rows_here = shrink.shape[0]
    kv = (r["kvacc"][...] + added[:, 2 * q_here :]).astype(jnp.bfloat16)
    cos_part, sin_part = r["rope_v"][0], r["rope_v"][1]

    def rotate(v):
        return (v * cos_part + pltpu.roll(v, HEAD_SIZE // 2, 1) * sin_part).astype(jnp.bfloat16)

    keys = rotate(kv[:, :HEAD_SIZE].astype(jnp.float32))
    values = kv[:, HEAD_SIZE:]
    up_to(choose, n)
    heads = 2 * q_here // HEAD_SIZE
    length = r["lengths"][0]
    line = lax.broadcasted_iota(jnp.int32, (rows_here, rows_here), 0)
    column = lax.broadcasted_iota(jnp.int32, (rows_here, rows_here), 1)
    allowed = (column <= line) & (column < length)
    for head in range(heads):
        at = slice(head * HEAD_SIZE, (head + 1) * HEAD_SIZE)
        query = rotate(r["qacc"][:, at] + added[:, at])
        scores = contract(query, keys) * HEAD_SIZE ** (-0.5)
        scores = jnp.where(allowed, scores, -1e30)
        highest = jnp.max(scores, axis=1, keepdims=True)
        expo = jnp.exp(scores - highest)
        weights = (expo / jnp.sum(expo, axis=1, keepdims=True)).astype(jnp.bfloat16)
        r["attended"][:, at] = mul(weights, values).astype(jnp.bfloat16)
    low = contract(r["attended"][...], r["out_down"][...]).astype(jnp.bfloat16)
    tile = min(512, width)

    @pl.loop(0, width // tile)
    def _(block):
        cols = pl.ds(pl.multiple_of(block * tile, tile), tile)
        base = jnp.zeros((rows_here, tile), jnp.float32)
        for half in range(2):
            term = mul(r["attended"][:, half * q_here : (half + 1) * q_here], r["wo"][half, :, cols])
            base = base + term.astype(jnp.bfloat16).astype(jnp.float32)
        r["base"][:, cols] = base

    valid = lax.broadcasted_iota(jnp.int32, (rows_here, 1), 0) < length
    span = r["up_all"].shape[-1]
    for number in range(UP_PIECES):
        up_to(pick, last_down + 1 + number)

        for half in range(2):
            at = (2 * number + half) * span
            cols = slice(at, at + span)
            total = r["base"][:, cols] + mul(low, r["up_all"][number, half])
            r["out"][:, cols] = jnp.where(valid, total, 0.0).astype(jnp.bfloat16)

    for index in range(n):
        copy_a(index).wait_send()

        @pl.when(is_end)
        def _():
            copy_b_own(index).wait_send()
            copy_b_relay(index).wait_send()

        @pl.when(is_hub)
        def _():
            for to in range(2 * levels):

                @pl.when(me != to)
                def _():
                    copy_c(index, col, to, pair).wait_send()

    for copy in (pair_tokens, pair_q, pair_kv, pair_wo, pair_small, pair_shrink):
        copy.wait_send()


def local(tokens, qw, kvw, ow, adm, aqu, akv, aod, aou, req, pool, lengths):
    size = lax.axis_size("serve")
    count, rank, out_width = aou.shape
    rows, width = tokens.shape
    q_here, kv_here = qw.shape[1], kvw.shape[1]
    levels = size // 2
    small_width = q_here + kv_here + q_here
    down_span, up_span = width // (2 * DOWN_PIECES), out_width // (2 * UP_PIECES)
    pieces = [("down", i) for i in range(DOWN_PIECES)]
    pieces.insert(0, ("small", 0))
    pieces += [("up", i) for i in range(UP_PIECES)]
    shapes = {
        "down": (adm.shape[1], down_span),
        "small": (rank // 2, small_width),
        "up": (rank, up_span),
    }
    bf16, f32 = jnp.bfloat16, jnp.float32
    scratch = {}
    for index, (family, _) in enumerate(pieces):
        lines, span = shapes[family]
        kinds = {
            "raw": (4 * count,), "give": (count,), "sends": (size,),
            "hubs": (2, levels // 2),
        }
        for kind, lead in kinds.items():
            scratch[f"{kind}{index}"] = pltpu.VMEM((*lead, lines, span), bf16)
    scratch.update(
        small_all=pltpu.VMEM((2, 2, rank // 2, small_width), bf16),
        up_all=pltpu.VMEM((UP_PIECES, 2, rank, up_span), bf16),
        x=pltpu.VMEM((2, rows, width), bf16),
        wq=pltpu.VMEM((qw.shape[0], 2 * q_here), bf16),
        wkv=pltpu.VMEM((kvw.shape[0], 2 * kv_here), bf16),
        wo=pltpu.VMEM((2, ow.shape[0], out_width), bf16),
        rope_v=pltpu.VMEM((2, rows, HEAD_SIZE), f32),
        qacc=pltpu.VMEM((rows, 2 * q_here), f32),
        kvacc=pltpu.VMEM((rows, 2 * kv_here), f32),
        shrink_own=pltpu.VMEM((rows, 128), f32),
        shrink_other=pltpu.VMEM((rows, 128), f32),
        up_maps=pltpu.VMEM((3 * rank, 2 * q_here + 2 * kv_here), bf16),
        out_down=pltpu.VMEM((rank, 2 * q_here), bf16),
        attended=pltpu.VMEM((rows, 2 * q_here), bf16),
        load_sem=pltpu.SemaphoreType.DMA((5 + 2 * len(pieces) + 6,)),
        hop_send=pltpu.SemaphoreType.DMA((3, len(pieces))),
        hop_recv=pltpu.SemaphoreType.DMA((3, len(pieces))),
        c_send=pltpu.SemaphoreType.DMA((len(pieces), size)),
        c_recv=pltpu.SemaphoreType.DMA((len(pieces), 2, levels // 2)),
        base=pltpu.VMEM((rows, out_width), f32),
        pair_send=pltpu.SemaphoreType.DMA((6,)),
        pair_recv=pltpu.SemaphoreType.DMA((6,)),
    )
    operands = ["req", "pool", "lengths", "tokens", "qw", "kvw", "ow", "adm", "aqu", "akv", "aod", "aou", "rope"]
    plan = dict(
        names=operands + ["out"] + list(scratch),
        levels=levels, count=count, rank=rank, width=width, q_here=q_here, kv_here=kv_here,
        pieces=pieces,
    )
    rope = jnp.asarray(rotary_tables(rows, HEAD_SIZE))
    smem = pl.BlockSpec(memory_space=pltpu.SMEM)
    hbm = pl.BlockSpec(memory_space=pl.ANY)
    return pl.pallas_call(
        functools.partial(kernel, plan),
        out_shape=jax.ShapeDtypeStruct((rows, out_width), bf16),
        in_specs=[smem] * 3 + [hbm] * 10,
        out_specs=pl.BlockSpec(memory_space=pltpu.VMEM),
        scratch_shapes=list(scratch.values()),
        compiler_params=pltpu.CompilerParams(
            collective_id=0, has_side_effects=True, vmem_limit_bytes=60 * 1024 * 1024
        ),
        name="routed_attention",
    )(req, pool, lengths, tokens, qw, kvw, ow, adm, aqu, akv, aod, aou, rope)


def solution(mesh):
    placed = (
        P(("group", "serve"), "tensor"),
        P(None, "tensor"),
        P(None, "tensor"),
        P("tensor", None),
        P(("group", "serve"), None, "tensor"),
        P(("group", "serve"), None, "tensor"),
        P(("group", "serve"), None, "tensor"),
        P(("group", "serve"), None, "tensor"),
        P(("group", "serve"), None, "tensor"),
        P("group"),
        P("group"),
        P(("group", "serve")),
    )
    return jax.shard_map(
        local,
        mesh=mesh,
        in_specs=placed,
        out_specs=P(("group", "serve"), "tensor"),
        check_vma=False,
    )
```

```python
import functools

import jax
import jax.numpy as jnp
import numpy as np
from jax import lax
from jax.experimental import pallas as pl
from jax.experimental.pallas import tpu as pltpu
from jax.sharding import PartitionSpec as P

HEAD_SIZE = 128
DOWN_PIECES = 8
UP_PIECES = 2
BASE_PIECES = 8
AHEAD = 2
LAG_C = 1
LAG_P = 3
CHOOSE_1 = 9
MESH = pl.DeviceIdType.MESH


def rotary_tables(rows, width):
    half = width // 2
    freqs = np.float32(500000.0) ** (-(np.arange(half, dtype=np.float32) * np.float32(2.0) / np.float32(width)))
    angles = np.arange(rows, dtype=np.float32)[:, None] * freqs.astype(np.float32)[None, :]
    cosine, sine = np.cos(angles), np.sin(angles)
    return np.stack(
        [np.concatenate([cosine, cosine], 1), np.concatenate([-sine, sine], 1)]
    ).astype(np.float32)


def hub_of(pair, levels):
    return 2 * pair + 1 if 2 * pair + 1 < levels // 2 else 2 * pair


def kernel(plan, *refs):
    r = dict(zip(plan["names"], refs))
    count, rank, levels = plan["count"], plan["rank"], plan["levels"]
    width, q_here, kv_here = plan["width"], plan["q_here"], plan["kv_here"]
    pieces = plan["pieces"]
    n = len(pieces)
    pairs = levels // 2
    group = lax.axis_index("group")
    me = lax.axis_index("serve")
    side = lax.axis_index("tensor")
    level = lax.div(me, 2)
    col = lax.rem(me, 2)
    pair = lax.div(level, 2)
    upper = jnp.where(2 * pair + 1 < pairs, 0, 1)
    is_hub = lax.rem(level, 2) != upper
    is_end = lax.rem(level, 2) == upper
    mate = level + 1 - 2 * lax.rem(level, 2)
    core_mate = (group, me, 1 - side)
    col_mate = (group, level * 2 + 1 - col, side)
    level_mate = (group, mate * 2 + col, side)

    def load(index, src, dst):
        return pltpu.make_async_copy(src, dst, r["load_sem"].at[index])

    own_q = pl.ds(pl.multiple_of(side * q_here, q_here), q_here)
    own_kv = pl.ds(pl.multiple_of(side * kv_here, kv_here), kv_here)
    own_cols = pl.ds(pl.multiple_of(side * width, width), width)
    other_cols = pl.ds(pl.multiple_of((1 - side) * width, width), width)
    loads = [
        load(0, r["tokens"], r["x"].at[side]),
        load(1, r["qw"], r["wq"].at[:, own_q]),
        load(2, r["kvw"], r["wkv"].at[:, own_kv]),
        load(3, r["ow"].at[:, own_cols], r["wo"].at[side]),
        load(4, r["rope"], r["rope_v"]),
    ]
    load_tokens, load_q, load_kv, load_wo, load_rope = loads
    tables = [
        pltpu.make_async_copy(r[name], r[name + "_s"], r["table_sem"].at[index])
        for index, name in enumerate(("req", "pool"))
    ]
    for copy in tables:
        copy.start()
    raw = [r[f"raw{index}"] for index in range(n)]
    give = [r[f"give{index}"] for index in range(n)]
    sends = [r[f"sends{index}"] for index in range(n)]
    hubs = [r[f"hubs{index}"] for index in range(n)]
    spans = [ref.shape[-1] for ref in give]
    piece_loads = []
    for index, (family, number) in enumerate(pieces):
        copies = []
        for slot, half, dst in ((0, col, raw[index].at[pl.ds(0, count)]), (1, 1 - col, give[index])):
            if family == "small":
                lines = pl.ds(pl.multiple_of(half * (rank // 2), rank // 2), rank // 2)
                at = 0
                for part, name in enumerate(("aqu", "akv", "aod")):
                    wide = r[name].shape[-1]
                    sem = len(loads) + 2 * n + 2 * part + slot
                    copies.append(load(sem, r[name].at[:, lines, :], dst.at[:, :, at : at + wide]))
                    at += wide
            else:
                src = r["adm" if family == "down" else "aou"]
                span = spans[index]
                at = pl.ds(pl.multiple_of((2 * number + half) * span, span), span)
                copies.append(load(len(loads) + 2 * index + slot, src.at[:, :, at], dst))
        piece_loads.append(copies)
    for copies in piece_loads:
        for copy in copies:
            copy.start()
    for copy in loads:
        copy.start()

    barrier = pltpu.get_barrier_semaphore()

    def greet(device):
        pl.semaphore_signal(barrier, inc=1, device_id=device, device_id_type=MESH)

    greet(core_mate)
    for other in range(2 * levels):
        other_hub = other // 2 == hub_of(other // 4, levels)

        @pl.when((me != other) if other_hub else ((me != other) & is_hub))
        def _():
            greet((group, other, side))

    @pl.when(is_end)
    def _():
        greet(col_mate)

    pl.semaphore_wait(barrier, jnp.where(is_hub, 2 * levels, 2 * pairs + 2))

    def remote(src, dst, send_sem, recv_sem, device):
        return pltpu.make_async_remote_copy(
            src_ref=src, dst_ref=dst, send_sem=send_sem, recv_sem=recv_sem,
            device_id=device, device_id_type=MESH,
        )

    def hop(kind, index, src, dst, device):
        return remote(src, dst, r["hop_send"].at[kind, index], r["hop_recv"].at[kind, index], device)

    def raws(index, at):
        return raw[index].at[pl.ds(at * count, count)]

    def copy_a(index):
        return hop(0, index, give[index], raws(index, 1), col_mate)

    def copy_b_own(index):
        return hop(1, index, raws(index, 0), raws(index, 2), level_mate)

    def copy_b_relay(index):
        return hop(2, index, raws(index, 1), raws(index, 3), level_mate)

    def copy_c(index, half, to, hub_pair):
        return remote(
            sends[index].at[to],
            hubs[index].at[half, hub_pair],
            r["c_send"].at[index, to],
            r["c_recv"].at[index, half, hub_pair],
            (group, to, side),
        )

    pair_copy = lambda index, src, dst: remote(
        src, dst, r["pair_send"].at[index], r["pair_recv"].at[index], core_mate
    )
    pair_tokens = pair_copy(0, r["tokens"], r["x"].at[side])
    pair_q = pair_copy(1, r["qw"], r["wq"].at[:, own_q])
    pair_kv = pair_copy(2, r["kvw"], r["wkv"].at[:, own_kv])
    pair_wo = pair_copy(3, r["ow"].at[:, other_cols], r["wo"].at[side])
    pair_small = pair_copy(4, r["small_all"].at[side], r["small_all"].at[side])
    pair_shrink = pair_copy(5, r["shrink_own"], r["shrink_other"])

    for copy in tables:
        copy.wait()

    def facts(target):
        wanted = r["pool_s"][r["req_s"][target]]
        owner = lax.div(wanted, count)
        owner_level = lax.div(owner, 2)
        away = jnp.where(lax.rem(owner_level, 2) == lax.rem(level, 2), 0, 2)
        aside = jnp.where(lax.rem(owner, 2) == col, 0, 1)
        return (away + aside) * count + wanted - owner * count, lax.div(owner_level, 2)

    mine = facts(me)
    wants = [facts(to) for to in range(2 * levels)]

    contract = lambda a, b: lax.dot_general(
        a, b, (((1,), (1,)), ((), ())), preferred_element_type=jnp.float32
    )
    mul = lambda a, b: jnp.dot(a, b, preferred_element_type=jnp.float32)
    three = 3 * rank

    def start(index):
        for copy in piece_loads[index]:
            copy.wait()
        copy_a(index).start()

        @pl.when(is_end)
        def _():
            copy_b_own(index).start()

    def relay(index):
        copy_a(index).wait_recv()

        @pl.when(is_end)
        def _():
            copy_b_relay(index).start()

    send_order = sorted(range(2 * levels), key=lambda to: -abs(2 * (to // 2) + 1 - levels))

    def choose(index):
        @pl.when(is_hub)
        def _():
            copy_b_own(index).wait_recv()
            copy_b_relay(index).wait_recv()
            for to in send_order:

                @pl.when(me != to)
                def _():
                    sends[index][to] = raw[index][wants[to][0]]
                    copy_c(index, col, to, pair).start()

            hubs[index][col, pair] = raw[index][mine[0]]

    def pick(index):
        family, number = pieces[index]
        for half in range(2):
            for hub in range(pairs):

                @pl.when(me != 2 * hub_of(hub, levels) + half)
                def _():
                    copy_c(index, half, 2 * hub_of(hub, levels) + half, hub).wait_recv()

        for half in range(2):
            value = hubs[index][half, mine[1]]
            if family == "down":
                at = (2 * number + half) * spans[index]
                x_part = r["x"][side, :, at : at + spans[index]]
                r["shrink_own"][:, :three] += contract(x_part, value)
            elif family == "small":
                r["small_all"][side, half] = value
            else:
                r["up_all"][number, half] = value
        if family == "small":
            pair_small.start()

    for index in range(AHEAD):
        start(index)
    for copy in (pair_tokens, pair_kv, pair_q, pair_wo):
        copy.start()

    r["qacc"][...] = jnp.zeros_like(r["qacc"])
    r["kvacc"][...] = jnp.zeros_like(r["kvacc"])
    r["shrink_own"][...] = jnp.zeros_like(r["shrink_own"])
    r["up_maps"][...] = jnp.zeros_like(r["up_maps"])

    def base_block(number):
        tile = width // BASE_PIECES
        for half in range(2):
            cols = pl.ds(pl.multiple_of(number * tile, tile), tile)
            rows = pl.ds(pl.multiple_of(half * width + number * tile, tile), tile)
            x_block = r["x"][half, :, cols]
            r["qacc"][...] += mul(x_block, r["wq"][rows, :])
            r["kvacc"][...] += mul(x_block, r["wkv"][rows, :])

    last_down = max(i for i, p in enumerate(pieces) if p[0] == "down")
    done = {start: AHEAD, relay: 0, choose: 0, pick: 0}
    lags = {start: -AHEAD, relay: 0, choose: LAG_C, pick: LAG_C + LAG_P}

    def up_to(action, index):
        while done[action] <= min(index, n - 1):
            action(done[action])
            done[action] += 1

    base_done = 0
    steps = last_down + lags[pick] + 1
    first_base = steps - 5
    for number in range(steps):
        for action in (start, relay, choose, pick):
            if action is pick and done[pick] == 0 and number == lags[pick]:
                load_tokens.wait()
            up_to(action, number - lags[action])
        if number == first_base:
            load_q.wait()
            load_kv.wait()
            for copy in (pair_tokens, pair_kv, pair_q):
                copy.wait_recv()
        if number >= first_base and base_done < BASE_PIECES:
            upto = min(BASE_PIECES, base_done + 2)

            @pl.loop(base_done, upto)
            def _(block):
                base_block(block)

            base_done = upto
    pair_shrink.start()

    up_to(relay, n)
    up_to(choose, CHOOSE_1)
    pair_small.wait_recv()
    lines = rank // 2
    for half in range(2):
        own = slice(half * q_here, (half + 1) * q_here)
        at = 2 * q_here + half * kv_here
        for part in range(2):
            small = r["small_all"][half, part]
            to = slice(part * lines, (part + 1) * lines)
            r["up_maps"][to, own] = small[:, :q_here]
            to_kv = slice((half + 1) * rank + part * lines, (half + 1) * rank + (part + 1) * lines)
            r["up_maps"][to_kv, at : at + kv_here] = small[:, q_here : q_here + kv_here]
            r["out_down"][to, own] = small[:, q_here + kv_here :]
    load_wo.wait()
    load_rope.wait()
    pair_wo.wait_recv()
    pair_shrink.wait_recv()

    shrink = (r["shrink_own"][:, :three] + r["shrink_other"][:, :three]).astype(jnp.bfloat16)
    added = mul(shrink, r["up_maps"][...])
    rows_here = shrink.shape[0]
    kv = (r["kvacc"][...] + added[:, 2 * q_here :]).astype(jnp.bfloat16)
    cos_part, sin_part = r["rope_v"][0], r["rope_v"][1]

    def rotate(v):
        return (v * cos_part + pltpu.roll(v, HEAD_SIZE // 2, 1) * sin_part).astype(jnp.bfloat16)

    keys = rotate(kv[:, :HEAD_SIZE].astype(jnp.float32))
    values = kv[:, HEAD_SIZE:]
    up_to(choose, n)
    heads = 2 * q_here // HEAD_SIZE
    length = r["lengths"][0]
    line = lax.broadcasted_iota(jnp.int32, (rows_here, rows_here), 0)
    column = lax.broadcasted_iota(jnp.int32, (rows_here, rows_here), 1)
    allowed = (column <= line) & (column < length)
    for head in range(heads):
        at = slice(head * HEAD_SIZE, (head + 1) * HEAD_SIZE)
        query = rotate(r["qacc"][:, at] + added[:, at])
        scores = contract(query, keys) * HEAD_SIZE ** (-0.5)
        scores = jnp.where(allowed, scores, -1e30)
        highest = jnp.max(scores, axis=1, keepdims=True)
        expo = jnp.exp(scores - highest)
        weights = (expo / jnp.sum(expo, axis=1, keepdims=True)).astype(jnp.bfloat16)
        r["attended"][:, at] = mul(weights, values).astype(jnp.bfloat16)
    low = contract(r["attended"][...], r["out_down"][...]).astype(jnp.bfloat16)
    tile = min(512, width)

    @pl.loop(0, width // tile)
    def _(block):
        cols = pl.ds(pl.multiple_of(block * tile, tile), tile)
        base = jnp.zeros((rows_here, tile), jnp.float32)
        for half in range(2):
            term = mul(r["attended"][:, half * q_here : (half + 1) * q_here], r["wo"][half, :, cols])
            base = base + term.astype(jnp.bfloat16).astype(jnp.float32)
        r["base"][:, cols] = base

    valid = lax.broadcasted_iota(jnp.int32, (rows_here, 1), 0) < length
    span = r["up_all"].shape[-1]
    for number in range(UP_PIECES):
        up_to(pick, last_down + 1 + number)

        for half in range(2):
            at = (2 * number + half) * span
            cols = slice(at, at + span)
            total = r["base"][:, cols] + mul(low, r["up_all"][number, half])
            r["out"][:, cols] = jnp.where(valid, total, 0.0).astype(jnp.bfloat16)

    for index in range(n):
        copy_a(index).wait_send()

        @pl.when(is_end)
        def _():
            copy_b_own(index).wait_send()
            copy_b_relay(index).wait_send()

        @pl.when(is_hub)
        def _():
            for to in range(2 * levels):

                @pl.when(me != to)
                def _():
                    copy_c(index, col, to, pair).wait_send()

    for copy in (pair_tokens, pair_q, pair_kv, pair_wo, pair_small, pair_shrink):
        copy.wait_send()


def local(tokens, qw, kvw, ow, adm, aqu, akv, aod, aou, req, pool, lengths):
    size = lax.axis_size("serve")
    count, rank, out_width = aou.shape
    rows, width = tokens.shape
    q_here, kv_here = qw.shape[1], kvw.shape[1]
    levels = size // 2
    small_width = q_here + kv_here + q_here
    down_span, up_span = width // (2 * DOWN_PIECES), out_width // (2 * UP_PIECES)
    pieces = [("down", i) for i in range(DOWN_PIECES)]
    pieces.insert(0, ("small", 0))
    pieces += [("up", i) for i in range(UP_PIECES)]
    shapes = {
        "down": (adm.shape[1], down_span),
        "small": (rank // 2, small_width),
        "up": (rank, up_span),
    }
    bf16, f32 = jnp.bfloat16, jnp.float32
    scratch = {}
    for index, (family, _) in enumerate(pieces):
        lines, span = shapes[family]
        kinds = {
            "raw": (4 * count,), "give": (count,), "sends": (size,),
            "hubs": (2, levels // 2),
        }
        for kind, lead in kinds.items():
            scratch[f"{kind}{index}"] = pltpu.VMEM((*lead, lines, span), bf16)
    scratch.update(
        small_all=pltpu.VMEM((2, 2, rank // 2, small_width), bf16),
        up_all=pltpu.VMEM((UP_PIECES, 2, rank, up_span), bf16),
        x=pltpu.VMEM((2, rows, width), bf16),
        wq=pltpu.VMEM((qw.shape[0], 2 * q_here), bf16),
        wkv=pltpu.VMEM((kvw.shape[0], 2 * kv_here), bf16),
        wo=pltpu.VMEM((2, ow.shape[0], out_width), bf16),
        rope_v=pltpu.VMEM((2, rows, HEAD_SIZE), f32),
        qacc=pltpu.VMEM((rows, 2 * q_here), f32),
        kvacc=pltpu.VMEM((rows, 2 * kv_here), f32),
        shrink_own=pltpu.VMEM((rows, 128), f32),
        shrink_other=pltpu.VMEM((rows, 128), f32),
        up_maps=pltpu.VMEM((3 * rank, 2 * q_here + 2 * kv_here), bf16),
        out_down=pltpu.VMEM((rank, 2 * q_here), bf16),
        attended=pltpu.VMEM((rows, 2 * q_here), bf16),
        req_s=pltpu.SMEM(req.shape, jnp.int32),
        pool_s=pltpu.SMEM(pool.shape, jnp.int32),
        table_sem=pltpu.SemaphoreType.DMA((2,)),
        load_sem=pltpu.SemaphoreType.DMA((5 + 2 * len(pieces) + 6,)),
        hop_send=pltpu.SemaphoreType.DMA((3, len(pieces))),
        hop_recv=pltpu.SemaphoreType.DMA((3, len(pieces))),
        c_send=pltpu.SemaphoreType.DMA((len(pieces), size)),
        c_recv=pltpu.SemaphoreType.DMA((len(pieces), 2, levels // 2)),
        base=pltpu.VMEM((rows, out_width), f32),
        pair_send=pltpu.SemaphoreType.DMA((6,)),
        pair_recv=pltpu.SemaphoreType.DMA((6,)),
    )
    operands = ["lengths", "req", "pool", "tokens", "qw", "kvw", "ow", "adm", "aqu", "akv", "aod", "aou", "rope"]
    plan = dict(
        names=operands + ["out"] + list(scratch),
        levels=levels, count=count, rank=rank, width=width, q_here=q_here, kv_here=kv_here,
        pieces=pieces,
    )
    rope = jnp.asarray(rotary_tables(rows, HEAD_SIZE))
    arrays = (req, pool, tokens, qw, kvw, ow, adm, aqu, akv, aod, aou, rope)
    hbm = pl.BlockSpec(memory_space=pl.ANY)
    return pl.pallas_call(
        functools.partial(kernel, plan),
        out_shape=jax.ShapeDtypeStruct((rows, out_width), bf16),
        in_specs=[pl.BlockSpec(memory_space=pltpu.SMEM)] + [hbm] * len(arrays),
        out_specs=pl.BlockSpec(memory_space=pltpu.VMEM),
        scratch_shapes=list(scratch.values()),
        compiler_params=pltpu.CompilerParams(
            collective_id=0, has_side_effects=True, vmem_limit_bytes=50 * 1024 * 1024
        ),
        name="routed_attention",
    )(lengths, *[pltpu.with_memory_space_constraint(array, pltpu.HBM) for array in arrays])


def solution(mesh):
    placed = (
        P(("group", "serve"), "tensor"),
        P(None, "tensor"),
        P(None, "tensor"),
        P("tensor", None),
        P(("group", "serve"), None, "tensor"),
        P(("group", "serve"), None, "tensor"),
        P(("group", "serve"), None, "tensor"),
        P(("group", "serve"), None, "tensor"),
        P(("group", "serve"), None, "tensor"),
        P("group"),
        P("group"),
        P(("group", "serve")),
    )
    return jax.shard_map(
        local,
        mesh=mesh,
        in_specs=placed,
        out_specs=P(("group", "serve"), "tensor"),
        check_vma=False,
    )
```

```python
import functools

import jax
import jax.numpy as jnp
import numpy as np
from jax import lax
from jax.experimental import pallas as pl
from jax.experimental.pallas import tpu as pltpu
from jax.sharding import PartitionSpec as P

HEAD_SIZE = 128
DOWN_PARTS = (2, 2, 2, 2, 2, 2, 2, 2)
UP_PARTS = (6, 6, 4)
BASE_PIECES = 8
AHEAD_A = 2
AHEAD_B = 1
LAG_C = 1
LAG_P = 3
EARLY = 2
TAIL = (2,)
MESH = pl.DeviceIdType.MESH


def rotary_tables(rows, width):
    half = width // 2
    freqs = np.float32(500000.0) ** (-(np.arange(half, dtype=np.float32) * np.float32(2.0) / np.float32(width)))
    angles = np.arange(rows, dtype=np.float32)[:, None] * freqs.astype(np.float32)[None, :]
    cosine, sine = np.cos(angles), np.sin(angles)
    return np.stack(
        [np.concatenate([cosine, cosine], 1), np.concatenate([-sine, sine], 1)]
    ).astype(np.float32)


def hub_of(pair, levels):
    return 2 * pair + 1 if 2 * pair + 1 < levels // 2 else 2 * pair


def kernel(plan, *refs):
    r = dict(zip(plan["names"], refs))
    count, rank, levels = plan["count"], plan["rank"], plan["levels"]
    width, q_here, kv_here = plan["width"], plan["q_here"], plan["kv_here"]
    pieces = plan["pieces"]
    n = len(pieces)
    pairs = levels // 2
    group = lax.axis_index("group")
    me = lax.axis_index("serve")
    side = lax.axis_index("tensor")
    level = lax.div(me, 2)
    col = lax.rem(me, 2)
    pair = lax.div(level, 2)
    upper = jnp.where(2 * pair + 1 < pairs, 0, 1)
    is_hub = lax.rem(level, 2) != upper
    is_end = lax.rem(level, 2) == upper
    mate = level + 1 - 2 * lax.rem(level, 2)
    core_mate = (group, me, 1 - side)
    col_mate = (group, level * 2 + 1 - col, side)
    level_mate = (group, mate * 2 + col, side)

    def load(index, src, dst):
        return pltpu.make_async_copy(src, dst, r["load_sem"].at[index])

    own_q = pl.ds(pl.multiple_of(side * q_here, q_here), q_here)
    own_kv = pl.ds(pl.multiple_of(side * kv_here, kv_here), kv_here)
    own_cols = pl.ds(pl.multiple_of(side * width, width), width)
    other_cols = pl.ds(pl.multiple_of((1 - side) * width, width), width)
    loads = [
        load(0, r["tokens"], r["x"].at[side]),
        load(1, r["qw"], r["wq"].at[:, own_q]),
        load(2, r["kvw"], r["wkv"].at[:, own_kv]),
        load(3, r["ow"].at[:, own_cols], r["wo"].at[side]),
        load(4, r["rope"], r["rope_v"]),
    ]
    load_tokens, load_q, load_kv, load_wo, load_rope = loads
    tables = [
        pltpu.make_async_copy(r[name], r[name + "_s"], r["table_sem"].at[index])
        for index, name in enumerate(("req", "pool"))
    ]
    for copy in tables:
        copy.start()
    raw = [r[f"raw{index}"] for index in range(n)]
    give = [r[f"give{index}"] for index in range(n)]
    sends = [r[f"sends{index}"] for index in range(n)]
    hubs = [r[f"hubs{index}"] for index in range(n)]
    spans = [ref.shape[-1] for ref in give]
    piece_loads = []
    for index, (family, number) in enumerate(pieces):
        copies = []
        for slot, half, dst in ((0, col, raw[index].at[pl.ds(0, count)]), (1, 1 - col, give[index])):
            if family == "small":
                lines = pl.ds(pl.multiple_of(half * (rank // 2), rank // 2), rank // 2)
                at = 0
                for part, name in enumerate(("aqu", "akv", "aod")):
                    wide = r[name].shape[-1]
                    sem = len(loads) + 2 * n + 2 * part + slot
                    copies.append(load(sem, r[name].at[:, lines, :], dst.at[:, :, at : at + wide]))
                    at += wide
            else:
                src = r["adm" if family == "down" else "aou"]
                span = spans[index]
                at = pl.ds(pl.multiple_of(number + half * span, 128), span)
                copies.append(load(len(loads) + 2 * index + slot, src.at[:, :, at], dst))
        piece_loads.append(copies)
    for copies in piece_loads:
        for copy in copies:
            copy.start()
    for copy in loads:
        copy.start()

    barrier = pltpu.get_barrier_semaphore()

    def greet(device):
        pl.semaphore_signal(barrier, inc=1, device_id=device, device_id_type=MESH)

    for device in (core_mate, col_mate, level_mate):
        greet(device)

    def other_hubs(action):
        for other in range(pairs):

            @pl.when(is_hub & (pair != other))
            def _():
                action((group, 2 * hub_of(other, levels) + col, side))

    other_hubs(greet)
    pl.semaphore_wait(barrier, jnp.where(is_hub, pairs + 2, 3))

    @pl.when(is_hub)
    def _():
        pl.semaphore_signal(r["met"], inc=1, device_id=col_mate, device_id_type=MESH)

    def meet():
        @pl.when(is_hub)
        def _():
            pl.semaphore_wait(r["met"], 1)

        other_hubs(
            lambda device: pl.semaphore_signal(
                r["met_hubs"], inc=1, device_id=device, device_id_type=MESH
            )
        )

        @pl.when(is_hub)
        def _():
            pl.semaphore_wait(r["met_hubs"], pairs - 1)

    def remote(src, dst, send_sem, recv_sem, device):
        return pltpu.make_async_remote_copy(
            src_ref=src, dst_ref=dst, send_sem=send_sem, recv_sem=recv_sem,
            device_id=device, device_id_type=MESH,
        )

    def hop(kind, index, src, dst, device):
        return remote(src, dst, r["hop_send"].at[kind, index], r["hop_recv"].at[kind, index], device)

    def raws(index, at):
        return raw[index].at[pl.ds(at * count, count)]

    def copy_a(index):
        return hop(0, index, give[index], raws(index, 1), col_mate)

    def copy_b_own(index):
        return hop(1, index, raws(index, 0), raws(index, 2), level_mate)

    def copy_b_relay(index):
        return hop(2, index, raws(index, 1), raws(index, 3), level_mate)

    def copy_c(index, half, to, hub_pair):
        return remote(
            sends[index].at[to],
            hubs[index].at[half, hub_pair],
            r["c_send"].at[index, to],
            r["c_recv"].at[index, half, hub_pair],
            (group, to, side),
        )

    pair_copy = lambda index, src, dst: remote(
        src, dst, r["pair_send"].at[index], r["pair_recv"].at[index], core_mate
    )
    pair_tokens = pair_copy(0, r["tokens"], r["x"].at[side])
    pair_q = pair_copy(1, r["qw"], r["wq"].at[:, own_q])
    pair_kv = pair_copy(2, r["kvw"], r["wkv"].at[:, own_kv])
    pair_wo = pair_copy(3, r["ow"].at[:, other_cols], r["wo"].at[side])
    pair_small = pair_copy(4, r["small_all"].at[side], r["small_all"].at[side])
    pair_shrink = pair_copy(5, r["shrink_own"], r["shrink_other"])

    for copy in tables:
        copy.wait()

    def facts(target):
        wanted = r["pool_s"][r["req_s"][target]]
        owner = lax.div(wanted, count)
        owner_level = lax.div(owner, 2)
        away = jnp.where(lax.rem(owner_level, 2) == lax.rem(level, 2), 0, 2)
        aside = jnp.where(lax.rem(owner, 2) == col, 0, 1)
        return (away + aside) * count + wanted - owner * count, lax.div(owner_level, 2)

    mine = facts(me)
    wants = [facts(to) for to in range(2 * levels)]

    contract = lambda a, b: lax.dot_general(
        a, b, (((1,), (1,)), ((), ())), preferred_element_type=jnp.float32
    )
    mul = lambda a, b: jnp.dot(a, b, preferred_element_type=jnp.float32)
    three = 3 * rank

    def start_a(index):
        for copy in piece_loads[index]:
            copy.wait()
        copy_a(index).start()

    def start_b(index):
        @pl.when(is_end)
        def _():
            copy_b_own(index).start()

    def relay(index):
        copy_a(index).wait_recv()

        @pl.when(is_end)
        def _():
            copy_b_relay(index).start()

    send_order = sorted(range(2 * levels), key=lambda to: -abs(2 * (to // 2) + 1 - levels))

    def choose(index):
        @pl.when(is_hub)
        def _():
            copy_b_own(index).wait_recv()
            copy_b_relay(index).wait_recv()
            for to in send_order:

                @pl.when(me != to)
                def _():
                    sends[index][to] = raw[index][wants[to][0]]
                    copy_c(index, col, to, pair).start()

            hubs[index][col, pair] = raw[index][mine[0]]

    def pick(index):
        family, number = pieces[index]
        for half in range(2):
            for hub in range(pairs):

                @pl.when(me != 2 * hub_of(hub, levels) + half)
                def _():
                    copy_c(index, half, 2 * hub_of(hub, levels) + half, hub).wait_recv()

        for half in range(2):
            value = hubs[index][half, mine[1]]
            if family == "down":
                at = number + half * spans[index]
                x_part = r["x"][side, :, at : at + spans[index]]
                r["shrink_own"][:, :three] += contract(x_part, value)
            elif family == "small":
                r["small_all"][side, half] = value
            else:
                at = number + half * spans[index]
                r["up_all"][:, at : at + spans[index]] = value
        if family == "small":
            pair_small.start()

    done = {start_a: 0, start_b: 0, relay: 0, choose: 0, pick: 0}
    lags = {start_a: -AHEAD_A, start_b: -AHEAD_B, relay: 0, choose: LAG_C, pick: LAG_C + LAG_P}

    def up_to(action, index):
        while done[action] <= min(index, n - 1):
            action(done[action])
            done[action] += 1

    for index in range(AHEAD_A):
        up_to(start_a, index)
        if index < AHEAD_B:
            up_to(start_b, index)
    for copy in (pair_tokens, pair_kv, pair_q, pair_wo):
        copy.start()
    meet()

    r["qacc"][...] = jnp.zeros_like(r["qacc"])
    r["kvacc"][...] = jnp.zeros_like(r["kvacc"])
    r["shrink_own"][...] = jnp.zeros_like(r["shrink_own"])
    r["up_maps"][...] = jnp.zeros_like(r["up_maps"])

    def base_block(number):
        tile = width // BASE_PIECES
        for half in range(2):
            cols = pl.ds(pl.multiple_of(number * tile, tile), tile)
            rows = pl.ds(pl.multiple_of(half * width + number * tile, tile), tile)
            x_block = r["x"][half, :, cols]
            r["qacc"][...] += mul(x_block, r["wq"][rows, :])
            r["kvacc"][...] += mul(x_block, r["wkv"][rows, :])

    last_down = max(i for i, p in enumerate(pieces) if p[0] == "down")
    base_done = 0
    steps = last_down + lags[pick] + 1
    first_base = steps - 5
    for number in range(steps):
        for action in (start_a, start_b, relay, choose, pick):
            if action is pick and done[pick] == 0 and number == lags[pick]:
                load_tokens.wait()
            limit = last_down + EARLY if action is choose else n
            up_to(action, min(number - lags[action], limit))
        if number == first_base:
            load_q.wait()
            load_kv.wait()
            for copy in (pair_tokens, pair_kv, pair_q):
                copy.wait_recv()
        if number >= first_base and base_done < BASE_PIECES:
            upto = min(BASE_PIECES, base_done + 2)

            @pl.loop(base_done, upto)
            def _(block):
                base_block(block)

            base_done = upto
    pair_shrink.start()

    def tail_point(point):
        up_to(relay, n)
        for at in TAIL:
            if at == point:
                up_to(choose, done[choose])

    tail_point(0)
    pair_small.wait_recv()
    lines = rank // 2
    for half in range(2):
        own = slice(half * q_here, (half + 1) * q_here)
        at = 2 * q_here + half * kv_here
        for part in range(2):
            small = r["small_all"][half, part]
            to = slice(part * lines, (part + 1) * lines)
            r["up_maps"][to, own] = small[:, :q_here]
            to_kv = slice((half + 1) * rank + part * lines, (half + 1) * rank + (part + 1) * lines)
            r["up_maps"][to_kv, at : at + kv_here] = small[:, q_here : q_here + kv_here]
            r["out_down"][to, own] = small[:, q_here + kv_here :]
    load_wo.wait()
    load_rope.wait()
    pair_wo.wait_recv()
    pair_shrink.wait_recv()
    tail_point(1)

    shrink = (r["shrink_own"][:, :three] + r["shrink_other"][:, :three]).astype(jnp.bfloat16)
    added = mul(shrink, r["up_maps"][...])
    rows_here = shrink.shape[0]
    kv = (r["kvacc"][...] + added[:, 2 * q_here :]).astype(jnp.bfloat16)
    cos_part, sin_part = r["rope_v"][0], r["rope_v"][1]

    def rotate(v):
        return (v * cos_part + pltpu.roll(v, HEAD_SIZE // 2, 1) * sin_part).astype(jnp.bfloat16)

    keys = rotate(kv[:, :HEAD_SIZE].astype(jnp.float32))
    values = kv[:, HEAD_SIZE:]
    tail_point(2)
    heads = 2 * q_here // HEAD_SIZE
    length = r["lengths"][0]
    line = lax.broadcasted_iota(jnp.int32, (rows_here, rows_here), 0)
    column = lax.broadcasted_iota(jnp.int32, (rows_here, rows_here), 1)
    allowed = (column <= line) & (column < length)
    for head in range(heads):
        at = slice(head * HEAD_SIZE, (head + 1) * HEAD_SIZE)
        query = rotate(r["qacc"][:, at] + added[:, at])
        scores = contract(query, keys) * HEAD_SIZE ** (-0.5)
        scores = jnp.where(allowed, scores, -1e30)
        highest = jnp.max(scores, axis=1, keepdims=True)
        expo = jnp.exp(scores - highest)
        weights = (expo / jnp.sum(expo, axis=1, keepdims=True)).astype(jnp.bfloat16)
        r["attended"][:, at] = mul(weights, values).astype(jnp.bfloat16)
        tail_point(3 + head)
    up_to(choose, n)
    low = contract(r["attended"][...], r["out_down"][...]).astype(jnp.bfloat16)
    tile = min(512, width)

    @pl.loop(0, width // tile)
    def _(block):
        cols = pl.ds(pl.multiple_of(block * tile, tile), tile)
        base = jnp.zeros((rows_here, tile), jnp.float32)
        for half in range(2):
            term = mul(r["attended"][:, half * q_here : (half + 1) * q_here], r["wo"][half, :, cols])
            base = base + term.astype(jnp.bfloat16).astype(jnp.float32)
        r["base"][:, cols] = base

    valid = lax.broadcasted_iota(jnp.int32, (rows_here, 1), 0) < length
    for index in range(last_down + 1, n):
        up_to(pick, index)
        for half in range(2):
            at = pieces[index][1] + half * spans[index]
            cols = slice(at, at + spans[index])
            total = r["base"][:, cols] + mul(low, r["up_all"][:, cols])
            r["out"][:, cols] = jnp.where(valid, total, 0.0).astype(jnp.bfloat16)

    for index in range(n):
        copy_a(index).wait_send()

        @pl.when(is_end)
        def _():
            copy_b_own(index).wait_send()
            copy_b_relay(index).wait_send()

        @pl.when(is_hub)
        def _():
            for to in range(2 * levels):

                @pl.when(me != to)
                def _():
                    copy_c(index, col, to, pair).wait_send()

    for copy in (pair_tokens, pair_q, pair_kv, pair_wo, pair_small, pair_shrink):
        copy.wait_send()


def local(tokens, qw, kvw, ow, adm, aqu, akv, aod, aou, req, pool, lengths):
    size = lax.axis_size("serve")
    count, rank, out_width = aou.shape
    rows, width = tokens.shape
    q_here, kv_here = qw.shape[1], kvw.shape[1]
    levels = size // 2
    small_width = q_here + kv_here + q_here
    pieces = [("small", 0, rank // 2, small_width)]
    for family, lines, whole, parts in (
        ("down", adm.shape[1], width, DOWN_PARTS),
        ("up", rank, out_width, UP_PARTS),
    ):
        unit = whole // (2 * sum(parts))
        for index, part in enumerate(parts):
            pieces.append((family, 2 * unit * sum(parts[:index]), lines, unit * part))
    bf16, f32 = jnp.bfloat16, jnp.float32
    scratch = {}
    for index, (_, _, lines, span) in enumerate(pieces):
        kinds = {
            "raw": (4 * count,), "give": (count,), "sends": (size,),
            "hubs": (2, levels // 2),
        }
        for kind, lead in kinds.items():
            scratch[f"{kind}{index}"] = pltpu.VMEM((*lead, lines, span), bf16)
    scratch.update(
        small_all=pltpu.VMEM((2, 2, rank // 2, small_width), bf16),
        up_all=pltpu.VMEM((rank, out_width), bf16),
        x=pltpu.VMEM((2, rows, width), bf16),
        wq=pltpu.VMEM((qw.shape[0], 2 * q_here), bf16),
        wkv=pltpu.VMEM((kvw.shape[0], 2 * kv_here), bf16),
        wo=pltpu.VMEM((2, ow.shape[0], out_width), bf16),
        rope_v=pltpu.VMEM((2, rows, HEAD_SIZE), f32),
        qacc=pltpu.VMEM((rows, 2 * q_here), f32),
        kvacc=pltpu.VMEM((rows, 2 * kv_here), f32),
        shrink_own=pltpu.VMEM((rows, 128), f32),
        shrink_other=pltpu.VMEM((rows, 128), f32),
        up_maps=pltpu.VMEM((3 * rank, 2 * q_here + 2 * kv_here), bf16),
        out_down=pltpu.VMEM((rank, 2 * q_here), bf16),
        attended=pltpu.VMEM((rows, 2 * q_here), bf16),
        req_s=pltpu.SMEM(req.shape, jnp.int32),
        pool_s=pltpu.SMEM(pool.shape, jnp.int32),
        met=pltpu.SemaphoreType.REGULAR,
        met_hubs=pltpu.SemaphoreType.REGULAR,
        table_sem=pltpu.SemaphoreType.DMA((2,)),
        load_sem=pltpu.SemaphoreType.DMA((5 + 2 * len(pieces) + 6,)),
        hop_send=pltpu.SemaphoreType.DMA((3, len(pieces))),
        hop_recv=pltpu.SemaphoreType.DMA((3, len(pieces))),
        c_send=pltpu.SemaphoreType.DMA((len(pieces), size)),
        c_recv=pltpu.SemaphoreType.DMA((len(pieces), 2, levels // 2)),
        base=pltpu.VMEM((rows, out_width), f32),
        pair_send=pltpu.SemaphoreType.DMA((6,)),
        pair_recv=pltpu.SemaphoreType.DMA((6,)),
    )
    operands = ["lengths", "req", "pool", "tokens", "qw", "kvw", "ow", "adm", "aqu", "akv", "aod", "aou", "rope"]
    plan = dict(
        names=operands + ["out"] + list(scratch),
        levels=levels, count=count, rank=rank, width=width, q_here=q_here, kv_here=kv_here,
        pieces=[piece[:2] for piece in pieces],
    )
    rope = jnp.asarray(rotary_tables(rows, HEAD_SIZE))
    arrays = (req, pool, tokens, qw, kvw, ow, adm, aqu, akv, aod, aou, rope)
    hbm = pl.BlockSpec(memory_space=pl.ANY)
    return pl.pallas_call(
        functools.partial(kernel, plan),
        out_shape=jax.ShapeDtypeStruct((rows, out_width), bf16),
        in_specs=[pl.BlockSpec(memory_space=pltpu.SMEM)] + [hbm] * len(arrays),
        out_specs=pl.BlockSpec(memory_space=pltpu.VMEM),
        scratch_shapes=list(scratch.values()),
        compiler_params=pltpu.CompilerParams(
            collective_id=0, has_side_effects=True, vmem_limit_bytes=50 * 1024 * 1024
        ),
        name="routed_attention",
    )(lengths, *[pltpu.with_memory_space_constraint(array, pltpu.HBM) for array in arrays])


def solution(mesh):
    placed = (
        P(("group", "serve"), "tensor"),
        P(None, "tensor"),
        P(None, "tensor"),
        P("tensor", None),
        P(("group", "serve"), None, "tensor"),
        P(("group", "serve"), None, "tensor"),
        P(("group", "serve"), None, "tensor"),
        P(("group", "serve"), None, "tensor"),
        P(("group", "serve"), None, "tensor"),
        P("group"),
        P("group"),
        P(("group", "serve")),
    )
    return jax.shard_map(
        local,
        mesh=mesh,
        in_specs=placed,
        out_specs=P(("group", "serve"), "tensor"),
        check_vma=False,
    )
```

```python
import functools

import jax
import jax.numpy as jnp
import numpy as np
from jax import lax
from jax.experimental import pallas as pl
from jax.experimental.pallas import tpu as pltpu
from jax.sharding import PartitionSpec as P

HEAD_SIZE = 128
DOWN_PARTS = (2, 2, 2, 2, 2, 2, 2, 2)
UP_PARTS = (8, 8)
BASE_PIECES = 8
AHEAD_A = 2
AHEAD_B = 0
FIRST_B = 2
LAG_C = 1
LAG_P = 3
EARLY = 2
TAIL = ()
MESH = pl.DeviceIdType.MESH


def rotary_tables(rows, width):
    half = width // 2
    freqs = np.float32(500000.0) ** (-(np.arange(half, dtype=np.float32) * np.float32(2.0) / np.float32(width)))
    angles = np.arange(rows, dtype=np.float32)[:, None] * freqs.astype(np.float32)[None, :]
    cosine, sine = np.cos(angles), np.sin(angles)
    return np.stack(
        [np.concatenate([cosine, cosine], 1), np.concatenate([-sine, sine], 1)]
    ).astype(np.float32)


def hub_of(pair, levels):
    return 2 * pair + 1 if 2 * pair + 1 < levels // 2 else 2 * pair


def kernel(plan, *refs):
    r = dict(zip(plan["names"], refs))
    count, rank, levels = plan["count"], plan["rank"], plan["levels"]
    width, q_here, kv_here = plan["width"], plan["q_here"], plan["kv_here"]
    pieces = plan["pieces"]
    n = len(pieces)
    pairs = levels // 2
    group = lax.axis_index("group")
    me = lax.axis_index("serve")
    side = lax.axis_index("tensor")
    level = lax.div(me, 2)
    col = lax.rem(me, 2)
    pair = lax.div(level, 2)
    upper = jnp.where(2 * pair + 1 < pairs, 0, 1)
    is_hub = lax.rem(level, 2) != upper
    is_end = lax.rem(level, 2) == upper
    mate = level + 1 - 2 * lax.rem(level, 2)
    core_mate = (group, me, 1 - side)
    col_mate = (group, level * 2 + 1 - col, side)
    level_mate = (group, mate * 2 + col, side)

    def load(index, src, dst):
        return pltpu.make_async_copy(src, dst, r["load_sem"].at[index])

    own_q = pl.ds(pl.multiple_of(side * q_here, q_here), q_here)
    own_kv = pl.ds(pl.multiple_of(side * kv_here, kv_here), kv_here)
    own_cols = pl.ds(pl.multiple_of(side * width, width), width)
    other_cols = pl.ds(pl.multiple_of((1 - side) * width, width), width)
    loads = [
        load(0, r["tokens"], r["x"].at[side]),
        load(1, r["qw"], r["wq"].at[:, own_q]),
        load(2, r["kvw"], r["wkv"].at[:, own_kv]),
        load(3, r["ow"].at[:, own_cols], r["wo"].at[side]),
        load(4, r["rope"], r["rope_v"]),
    ]
    load_tokens, load_q, load_kv, load_wo, load_rope = loads
    tables = [
        pltpu.make_async_copy(r[name], r[name + "_s"], r["table_sem"].at[index])
        for index, name in enumerate(("req", "pool"))
    ]
    for copy in tables:
        copy.start()
    raw = [r[f"raw{index}"] for index in range(n)]
    give = [r[f"give{index}"] for index in range(n)]
    sends = [r[f"sends{index}"] for index in range(n)]
    hubs = [r[f"hubs{index}"] for index in range(n)]
    spans = [ref.shape[-1] for ref in give]
    piece_loads = []
    for index, (family, number) in enumerate(pieces):
        copies = []
        for slot, half, dst in ((0, col, raw[index].at[pl.ds(0, count)]), (1, 1 - col, give[index])):
            if family == "small":
                lines = pl.ds(pl.multiple_of(half * (rank // 2), rank // 2), rank // 2)
                at = 0
                for part, name in enumerate(("aqu", "akv", "aod")):
                    wide = r[name].shape[-1]
                    sem = len(loads) + 2 * n + 2 * part + slot
                    copies.append(load(sem, r[name].at[:, lines, :], dst.at[:, :, at : at + wide]))
                    at += wide
            else:
                src = r["adm" if family == "down" else "aou"]
                span = spans[index]
                at = pl.ds(pl.multiple_of(number + half * span, 128), span)
                copies.append(load(len(loads) + 2 * index + slot, src.at[:, :, at], dst))
        piece_loads.append(copies)
    for copies in piece_loads:
        for copy in copies:
            copy.start()
    for copy in loads:
        copy.start()

    barrier = pltpu.get_barrier_semaphore()

    def greet(device):
        pl.semaphore_signal(barrier, inc=1, device_id=device, device_id_type=MESH)

    for device in (core_mate, col_mate, level_mate):
        greet(device)

    def other_hubs(action):
        for other in range(pairs):

            @pl.when(is_hub & (pair != other))
            def _():
                action((group, 2 * hub_of(other, levels) + col, side))

    other_hubs(greet)
    pl.semaphore_wait(barrier, jnp.where(is_hub, pairs + 2, 3))

    @pl.when(is_hub)
    def _():
        pl.semaphore_signal(r["met"], inc=1, device_id=col_mate, device_id_type=MESH)

    def meet():
        @pl.when(is_hub)
        def _():
            pl.semaphore_wait(r["met"], 1)

        other_hubs(
            lambda device: pl.semaphore_signal(
                r["met_hubs"], inc=1, device_id=device, device_id_type=MESH
            )
        )

        @pl.when(is_hub)
        def _():
            pl.semaphore_wait(r["met_hubs"], pairs - 1)

    def remote(src, dst, send_sem, recv_sem, device):
        return pltpu.make_async_remote_copy(
            src_ref=src, dst_ref=dst, send_sem=send_sem, recv_sem=recv_sem,
            device_id=device, device_id_type=MESH,
        )

    def hop(kind, index, src, dst, device):
        return remote(src, dst, r["hop_send"].at[kind, index], r["hop_recv"].at[kind, index], device)

    def raws(index, at):
        return raw[index].at[pl.ds(at * count, count)]

    def copy_a(index):
        return hop(0, index, give[index], raws(index, 1), col_mate)

    def copy_b_own(index):
        return hop(1, index, raws(index, 0), raws(index, 2), level_mate)

    def copy_b_relay(index):
        return hop(2, index, raws(index, 1), raws(index, 3), level_mate)

    def copy_c(index, half, to, hub_pair):
        return remote(
            sends[index].at[to],
            hubs[index].at[half, hub_pair],
            r["c_send"].at[index, to],
            r["c_recv"].at[index, half, hub_pair],
            (group, to, side),
        )

    pair_copy = lambda index, src, dst: remote(
        src, dst, r["pair_send"].at[index], r["pair_recv"].at[index], core_mate
    )
    pair_tokens = pair_copy(0, r["tokens"], r["x"].at[side])
    pair_q = pair_copy(1, r["qw"], r["wq"].at[:, own_q])
    pair_kv = pair_copy(2, r["kvw"], r["wkv"].at[:, own_kv])
    pair_wo = pair_copy(3, r["ow"].at[:, other_cols], r["wo"].at[side])
    pair_small = pair_copy(4, r["small_all"].at[side], r["small_all"].at[side])
    pair_shrink = pair_copy(5, r["shrink_own"], r["shrink_other"])

    for copy in tables:
        copy.wait()

    def facts(target):
        wanted = r["pool_s"][r["req_s"][target]]
        owner = lax.div(wanted, count)
        owner_level = lax.div(owner, 2)
        away = jnp.where(lax.rem(owner_level, 2) == lax.rem(level, 2), 0, 2)
        aside = jnp.where(lax.rem(owner, 2) == col, 0, 1)
        return (away + aside) * count + wanted - owner * count, lax.div(owner_level, 2)

    mine = facts(me)
    wants = [facts(to) for to in range(2 * levels)]

    contract = lambda a, b: lax.dot_general(
        a, b, (((1,), (1,)), ((), ())), preferred_element_type=jnp.float32
    )
    mul = lambda a, b: jnp.dot(a, b, preferred_element_type=jnp.float32)
    three = 3 * rank

    def start_a(index):
        for copy in piece_loads[index]:
            copy.wait()
        copy_a(index).start()

    def start_b(index):
        @pl.when(is_end)
        def _():
            copy_b_own(index).start()

    def relay(index):
        @pl.when(is_end)
        def _():
            copy_a(index).wait_recv()
            copy_b_relay(index).start()

    send_order = sorted(range(2 * levels), key=lambda to: -abs(2 * (to // 2) + 1 - levels))

    def choose(index):
        @pl.when(is_hub)
        def _():
            copy_a(index).wait_recv()
            copy_b_own(index).wait_recv()
            copy_b_relay(index).wait_recv()
            for to in send_order:

                @pl.when(me != to)
                def _():
                    sends[index][to] = raw[index][wants[to][0]]
                    copy_c(index, col, to, pair).start()

            hubs[index][col, pair] = raw[index][mine[0]]

    def pick(index):
        family, number = pieces[index]
        for half in range(2):
            for hub in range(pairs):

                @pl.when(me != 2 * hub_of(hub, levels) + half)
                def _():
                    copy_c(index, half, 2 * hub_of(hub, levels) + half, hub).wait_recv()

        for half in range(2):
            value = hubs[index][half, mine[1]]
            if family == "down":
                at = number + half * spans[index]
                x_part = r["x"][side, :, at : at + spans[index]]
                r["shrink_own"][:, :three] += contract(x_part, value)
            elif family == "small":
                r["small_all"][side, half] = value
            else:
                at = number + half * spans[index]
                r["up_all"][:, at : at + spans[index]] = value
        if family == "small":
            pair_small.start()

    done = {start_a: 0, start_b: 0, relay: 0, choose: 0, pick: 0}
    lags = {start_a: -AHEAD_A, start_b: -AHEAD_B, relay: 0, choose: LAG_C, pick: LAG_C + LAG_P}

    def up_to(action, index):
        while done[action] <= min(index, n - 1):
            action(done[action])
            done[action] += 1

    for index in range(AHEAD_A):
        up_to(start_a, index)
        if index < FIRST_B:
            up_to(start_b, index)
    for copy in (pair_tokens, pair_kv, pair_q, pair_wo):
        copy.start()
    meet()

    r["qacc"][...] = jnp.zeros_like(r["qacc"])
    r["kvacc"][...] = jnp.zeros_like(r["kvacc"])
    r["shrink_own"][...] = jnp.zeros_like(r["shrink_own"])
    r["up_maps"][...] = jnp.zeros_like(r["up_maps"])

    def base_block(number):
        tile = width // BASE_PIECES
        for half in range(2):
            cols = pl.ds(pl.multiple_of(number * tile, tile), tile)
            rows = pl.ds(pl.multiple_of(half * width + number * tile, tile), tile)
            x_block = r["x"][half, :, cols]
            r["qacc"][...] += mul(x_block, r["wq"][rows, :])
            r["kvacc"][...] += mul(x_block, r["wkv"][rows, :])

    last_down = max(i for i, p in enumerate(pieces) if p[0] == "down")
    base_done = 0
    steps = last_down + lags[pick] + 1
    first_base = steps - 5
    for number in range(steps):
        for action in (start_a, start_b, relay, choose, pick):
            if action is pick and done[pick] == 0 and number == lags[pick]:
                load_tokens.wait()
            limit = last_down + EARLY if action is choose else n
            up_to(action, min(number - lags[action], limit))
        if number == first_base:
            load_q.wait()
            load_kv.wait()
            for copy in (pair_tokens, pair_kv, pair_q):
                copy.wait_recv()
        if number >= first_base and base_done < BASE_PIECES:
            upto = min(BASE_PIECES, base_done + 2)

            @pl.loop(base_done, upto)
            def _(block):
                base_block(block)

            base_done = upto
    pair_shrink.start()

    def tail_point(point):
        up_to(relay, n)
        for at in TAIL:
            if at == point:
                up_to(choose, done[choose])

    tail_point(0)
    pair_small.wait_recv()
    lines = rank // 2
    for half in range(2):
        own = slice(half * q_here, (half + 1) * q_here)
        at = 2 * q_here + half * kv_here
        for part in range(2):
            small = r["small_all"][half, part]
            to = slice(part * lines, (part + 1) * lines)
            r["up_maps"][to, own] = small[:, :q_here]
            to_kv = slice((half + 1) * rank + part * lines, (half + 1) * rank + (part + 1) * lines)
            r["up_maps"][to_kv, at : at + kv_here] = small[:, q_here : q_here + kv_here]
            r["out_down"][to, own] = small[:, q_here + kv_here :]
    load_wo.wait()
    load_rope.wait()
    pair_wo.wait_recv()
    pair_shrink.wait_recv()
    tail_point(1)

    shrink = (r["shrink_own"][:, :three] + r["shrink_other"][:, :three]).astype(jnp.bfloat16)
    added = mul(shrink, r["up_maps"][...])
    rows_here = shrink.shape[0]
    kv = (r["kvacc"][...] + added[:, 2 * q_here :]).astype(jnp.bfloat16)
    cos_part, sin_part = r["rope_v"][0], r["rope_v"][1]

    def rotate(v):
        return (v * cos_part + pltpu.roll(v, HEAD_SIZE // 2, 1) * sin_part).astype(jnp.bfloat16)

    keys = rotate(kv[:, :HEAD_SIZE].astype(jnp.float32))
    values = kv[:, HEAD_SIZE:]
    tail_point(2)
    heads = 2 * q_here // HEAD_SIZE
    length = r["lengths"][0]
    line = lax.broadcasted_iota(jnp.int32, (rows_here, rows_here), 0)
    column = lax.broadcasted_iota(jnp.int32, (rows_here, rows_here), 1)
    allowed = (column <= line) & (column < length)
    for head in range(heads):
        at = slice(head * HEAD_SIZE, (head + 1) * HEAD_SIZE)
        query = rotate(r["qacc"][:, at] + added[:, at])
        scores = contract(query, keys) * HEAD_SIZE ** (-0.5)
        scores = jnp.where(allowed, scores, -1e30)
        highest = jnp.max(scores, axis=1, keepdims=True)
        expo = jnp.exp(scores - highest)
        weights = (expo / jnp.sum(expo, axis=1, keepdims=True)).astype(jnp.bfloat16)
        r["attended"][:, at] = mul(weights, values).astype(jnp.bfloat16)
        tail_point(3 + head)
    up_to(choose, n)
    low = contract(r["attended"][...], r["out_down"][...]).astype(jnp.bfloat16)
    tile = min(512, width)

    @pl.loop(0, width // tile)
    def _(block):
        cols = pl.ds(pl.multiple_of(block * tile, tile), tile)
        base = jnp.zeros((rows_here, tile), jnp.float32)
        for half in range(2):
            term = mul(r["attended"][:, half * q_here : (half + 1) * q_here], r["wo"][half, :, cols])
            base = base + term.astype(jnp.bfloat16).astype(jnp.float32)
        r["base"][:, cols] = base

    valid = lax.broadcasted_iota(jnp.int32, (rows_here, 1), 0) < length
    for index in range(last_down + 1, n):
        up_to(pick, index)
        for half in range(2):
            at = pieces[index][1] + half * spans[index]
            cols = slice(at, at + spans[index])
            total = r["base"][:, cols] + mul(low, r["up_all"][:, cols])
            r["out"][:, cols] = jnp.where(valid, total, 0.0).astype(jnp.bfloat16)

    for index in range(n):
        copy_a(index).wait_send()

        @pl.when(is_end)
        def _():
            copy_b_own(index).wait_send()
            copy_b_relay(index).wait_send()

        @pl.when(is_hub)
        def _():
            for to in range(2 * levels):

                @pl.when(me != to)
                def _():
                    copy_c(index, col, to, pair).wait_send()

    for copy in (pair_tokens, pair_q, pair_kv, pair_wo, pair_small, pair_shrink):
        copy.wait_send()


def local(tokens, qw, kvw, ow, adm, aqu, akv, aod, aou, req, pool, lengths):
    size = lax.axis_size("serve")
    count, rank, out_width = aou.shape
    rows, width = tokens.shape
    q_here, kv_here = qw.shape[1], kvw.shape[1]
    levels = size // 2
    small_width = q_here + kv_here + q_here
    pieces = [("small", 0, rank // 2, small_width)]
    for family, lines, whole, parts in (
        ("down", adm.shape[1], width, DOWN_PARTS),
        ("up", rank, out_width, UP_PARTS),
    ):
        unit = whole // (2 * sum(parts))
        for index, part in enumerate(parts):
            pieces.append((family, 2 * unit * sum(parts[:index]), lines, unit * part))
    bf16, f32 = jnp.bfloat16, jnp.float32
    scratch = {}
    for index, (_, _, lines, span) in enumerate(pieces):
        kinds = {
            "raw": (4 * count,), "give": (count,), "sends": (size,),
            "hubs": (2, levels // 2),
        }
        for kind, lead in kinds.items():
            scratch[f"{kind}{index}"] = pltpu.VMEM((*lead, lines, span), bf16)
    scratch.update(
        small_all=pltpu.VMEM((2, 2, rank // 2, small_width), bf16),
        up_all=pltpu.VMEM((rank, out_width), bf16),
        x=pltpu.VMEM((2, rows, width), bf16),
        wq=pltpu.VMEM((qw.shape[0], 2 * q_here), bf16),
        wkv=pltpu.VMEM((kvw.shape[0], 2 * kv_here), bf16),
        wo=pltpu.VMEM((2, ow.shape[0], out_width), bf16),
        rope_v=pltpu.VMEM((2, rows, HEAD_SIZE), f32),
        qacc=pltpu.VMEM((rows, 2 * q_here), f32),
        kvacc=pltpu.VMEM((rows, 2 * kv_here), f32),
        shrink_own=pltpu.VMEM((rows, 128), f32),
        shrink_other=pltpu.VMEM((rows, 128), f32),
        up_maps=pltpu.VMEM((3 * rank, 2 * q_here + 2 * kv_here), bf16),
        out_down=pltpu.VMEM((rank, 2 * q_here), bf16),
        attended=pltpu.VMEM((rows, 2 * q_here), bf16),
        req_s=pltpu.SMEM(req.shape, jnp.int32),
        pool_s=pltpu.SMEM(pool.shape, jnp.int32),
        met=pltpu.SemaphoreType.REGULAR,
        met_hubs=pltpu.SemaphoreType.REGULAR,
        table_sem=pltpu.SemaphoreType.DMA((2,)),
        load_sem=pltpu.SemaphoreType.DMA((5 + 2 * len(pieces) + 6,)),
        hop_send=pltpu.SemaphoreType.DMA((3, len(pieces))),
        hop_recv=pltpu.SemaphoreType.DMA((3, len(pieces))),
        c_send=pltpu.SemaphoreType.DMA((len(pieces), size)),
        c_recv=pltpu.SemaphoreType.DMA((len(pieces), 2, levels // 2)),
        base=pltpu.VMEM((rows, out_width), f32),
        pair_send=pltpu.SemaphoreType.DMA((6,)),
        pair_recv=pltpu.SemaphoreType.DMA((6,)),
    )
    operands = ["lengths", "req", "pool", "tokens", "qw", "kvw", "ow", "adm", "aqu", "akv", "aod", "aou", "rope"]
    plan = dict(
        names=operands + ["out"] + list(scratch),
        levels=levels, count=count, rank=rank, width=width, q_here=q_here, kv_here=kv_here,
        pieces=[piece[:2] for piece in pieces],
    )
    rope = jnp.asarray(rotary_tables(rows, HEAD_SIZE))
    arrays = (req, pool, tokens, qw, kvw, ow, adm, aqu, akv, aod, aou, rope)
    hbm = pl.BlockSpec(memory_space=pl.ANY)
    return pl.pallas_call(
        functools.partial(kernel, plan),
        out_shape=jax.ShapeDtypeStruct((rows, out_width), bf16),
        in_specs=[pl.BlockSpec(memory_space=pltpu.SMEM)] + [hbm] * len(arrays),
        out_specs=pl.BlockSpec(memory_space=pltpu.VMEM),
        scratch_shapes=list(scratch.values()),
        compiler_params=pltpu.CompilerParams(
            collective_id=0, has_side_effects=True, vmem_limit_bytes=50 * 1024 * 1024
        ),
        name="routed_attention",
    )(lengths, *[pltpu.with_memory_space_constraint(array, pltpu.HBM) for array in arrays])


def solution(mesh):
    placed = (
        P(("group", "serve"), "tensor"),
        P(None, "tensor"),
        P(None, "tensor"),
        P("tensor", None),
        P(("group", "serve"), None, "tensor"),
        P(("group", "serve"), None, "tensor"),
        P(("group", "serve"), None, "tensor"),
        P(("group", "serve"), None, "tensor"),
        P(("group", "serve"), None, "tensor"),
        P("group"),
        P("group"),
        P(("group", "serve")),
    )
    return jax.shard_map(
        local,
        mesh=mesh,
        in_specs=placed,
        out_specs=P(("group", "serve"), "tensor"),
        check_vma=False,
    )
```

```python
import functools

import jax
import jax.numpy as jnp
import numpy as np
from jax import lax
from jax.experimental import pallas as pl
from jax.experimental.pallas import tpu as pltpu
from jax.sharding import PartitionSpec as P

HEAD_SIZE = 128
DOWN_PARTS = (2, 2, 2, 2, 2, 2, 2, 2)
UP_PARTS = (8, 8)
BASE_PIECES = 8
AHEAD_A = 2
AHEAD_B = 0
FIRST_B = 2
LAG_C = 1
LAG_P = 3
EARLY = 2
TAIL = ()
MESH = pl.DeviceIdType.MESH


def rotary_tables(rows, width):
    half = width // 2
    freqs = np.float32(500000.0) ** (-(np.arange(half, dtype=np.float32) * np.float32(2.0) / np.float32(width)))
    angles = np.arange(rows, dtype=np.float32)[:, None] * freqs.astype(np.float32)[None, :]
    cosine, sine = np.cos(angles), np.sin(angles)
    return np.stack(
        [np.concatenate([cosine, cosine], 1), np.concatenate([-sine, sine], 1)]
    ).astype(np.float32)


def hub_of(pair, levels):
    return 2 * pair + 1 if 2 * pair + 1 < levels // 2 else 2 * pair


def kernel(plan, *refs):
    r = dict(zip(plan["names"], refs))
    count, rank, levels = plan["count"], plan["rank"], plan["levels"]
    width, q_here, kv_here = plan["width"], plan["q_here"], plan["kv_here"]
    pieces = plan["pieces"]
    n = len(pieces)
    pairs = levels // 2
    group = lax.axis_index("group")
    me = lax.axis_index("serve")
    side = lax.axis_index("tensor")
    level = lax.div(me, 2)
    col = lax.rem(me, 2)
    pair = lax.div(level, 2)
    upper = jnp.where(2 * pair + 1 < pairs, 0, 1)
    is_hub = lax.rem(level, 2) != upper
    is_end = lax.rem(level, 2) == upper
    mate = level + 1 - 2 * lax.rem(level, 2)
    core_mate = (group, me, 1 - side)
    col_mate = (group, level * 2 + 1 - col, side)
    level_mate = (group, mate * 2 + col, side)

    barrier = pltpu.get_barrier_semaphore()

    def greet(device):
        pl.semaphore_signal(barrier, inc=1, device_id=device, device_id_type=MESH)

    for device in (core_mate, col_mate, level_mate):
        greet(device)

    def other_hubs(action):
        for other in range(pairs):

            @pl.when(is_hub & (pair != other))
            def _():
                action((group, 2 * hub_of(other, levels) + col, side))

    other_hubs(greet)
    def load(index, src, dst):
        return pltpu.make_async_copy(src, dst, r["load_sem"].at[index])

    own_q = pl.ds(pl.multiple_of(side * q_here, q_here), q_here)
    own_kv = pl.ds(pl.multiple_of(side * kv_here, kv_here), kv_here)
    own_cols = pl.ds(pl.multiple_of(side * width, width), width)
    other_cols = pl.ds(pl.multiple_of((1 - side) * width, width), width)
    loads = [
        load(0, r["tokens"], r["x"].at[side]),
        load(1, r["qw"], r["wq"].at[:, own_q]),
        load(2, r["kvw"], r["wkv"].at[:, own_kv]),
        load(3, r["ow"].at[:, own_cols], r["wo"].at[side]),
        load(4, r["rope"], r["rope_v"]),
    ]
    load_tokens, load_q, load_kv, load_wo, load_rope = loads
    tables = [
        pltpu.make_async_copy(r[name], r[name + "_s"], r["table_sem"].at[index])
        for index, name in enumerate(("req", "pool"))
    ]
    for copy in tables:
        copy.start()
    raw = [r[f"raw{index}"] for index in range(n)]
    give = [r[f"give{index}"] for index in range(n)]
    sends = [r[f"sends{index}"] for index in range(n)]
    hubs = [r[f"hubs{index}"] for index in range(n)]
    spans = [ref.shape[-1] for ref in give]
    piece_loads = []
    for index, (family, number) in enumerate(pieces):
        copies = []
        for slot, half, dst in ((0, col, raw[index].at[pl.ds(0, count)]), (1, 1 - col, give[index])):
            if family == "small":
                lines = pl.ds(pl.multiple_of(half * (rank // 2), rank // 2), rank // 2)
                at = 0
                for part, name in enumerate(("aqu", "akv", "aod")):
                    wide = r[name].shape[-1]
                    sem = len(loads) + 2 * n + 2 * part + slot
                    copies.append(load(sem, r[name].at[:, lines, :], dst.at[:, :, at : at + wide]))
                    at += wide
            else:
                src = r["adm" if family == "down" else "aou"]
                span = spans[index]
                at = pl.ds(pl.multiple_of(number + half * span, 128), span)
                copies.append(load(len(loads) + 2 * index + slot, src.at[:, :, at], dst))
        piece_loads.append(copies)
    for copies in piece_loads:
        for copy in copies:
            copy.start()
    for copy in loads:
        copy.start()

    pl.semaphore_wait(barrier, jnp.where(is_hub, pairs + 2, 3))

    @pl.when(is_hub)
    def _():
        pl.semaphore_signal(r["met"], inc=1, device_id=col_mate, device_id_type=MESH)

    def meet():
        @pl.when(is_hub)
        def _():
            pl.semaphore_wait(r["met"], 1)

        other_hubs(
            lambda device: pl.semaphore_signal(
                r["met_hubs"], inc=1, device_id=device, device_id_type=MESH
            )
        )

        @pl.when(is_hub)
        def _():
            pl.semaphore_wait(r["met_hubs"], pairs - 1)

    def remote(src, dst, send_sem, recv_sem, device):
        return pltpu.make_async_remote_copy(
            src_ref=src, dst_ref=dst, send_sem=send_sem, recv_sem=recv_sem,
            device_id=device, device_id_type=MESH,
        )

    def hop(kind, index, src, dst, device):
        return remote(src, dst, r["hop_send"].at[kind, index], r["hop_recv"].at[kind, index], device)

    def raws(index, at):
        return raw[index].at[pl.ds(at * count, count)]

    def copy_a(index):
        return hop(0, index, give[index], raws(index, 1), col_mate)

    def copy_b_own(index):
        return hop(1, index, raws(index, 0), raws(index, 2), level_mate)

    def copy_b_relay(index):
        return hop(2, index, raws(index, 1), raws(index, 3), level_mate)

    def copy_c(index, half, to, hub_pair):
        return remote(
            sends[index].at[to],
            hubs[index].at[half, hub_pair],
            r["c_send"].at[index, to],
            r["c_recv"].at[index, half, hub_pair],
            (group, to, side),
        )

    pair_copy = lambda index, src, dst: remote(
        src, dst, r["pair_send"].at[index], r["pair_recv"].at[index], core_mate
    )
    pair_tokens = pair_copy(0, r["tokens"], r["x"].at[side])
    pair_q = pair_copy(1, r["qw"], r["wq"].at[:, own_q])
    pair_kv = pair_copy(2, r["kvw"], r["wkv"].at[:, own_kv])
    pair_wo = pair_copy(3, r["ow"].at[:, other_cols], r["wo"].at[side])
    pair_small = pair_copy(4, r["small_all"].at[side], r["small_all"].at[side])
    pair_shrink = pair_copy(5, r["shrink_own"], r["shrink_other"])

    for copy in tables:
        copy.wait()

    def facts(target):
        wanted = r["pool_s"][r["req_s"][target]]
        owner = lax.div(wanted, count)
        owner_level = lax.div(owner, 2)
        away = jnp.where(lax.rem(owner_level, 2) == lax.rem(level, 2), 0, 2)
        aside = jnp.where(lax.rem(owner, 2) == col, 0, 1)
        return (away + aside) * count + wanted - owner * count, lax.div(owner_level, 2)

    mine = facts(me)
    wants = [facts(to) for to in range(2 * levels)]

    contract = lambda a, b: lax.dot_general(
        a, b, (((1,), (1,)), ((), ())), preferred_element_type=jnp.float32
    )
    mul = lambda a, b: jnp.dot(a, b, preferred_element_type=jnp.float32)
    three = 3 * rank

    def start_a(index):
        for copy in piece_loads[index]:
            copy.wait()
        copy_a(index).start()

    def start_b(index):
        @pl.when(is_end)
        def _():
            copy_b_own(index).start()

    def relay(index):
        @pl.when(is_end)
        def _():
            copy_a(index).wait_recv()
            copy_b_relay(index).start()

    send_order = sorted(range(2 * levels), key=lambda to: -abs(2 * (to // 2) + 1 - levels))

    def choose(index):
        @pl.when(is_hub)
        def _():
            copy_a(index).wait_recv()
            copy_b_own(index).wait_recv()
            copy_b_relay(index).wait_recv()
            for to in send_order:

                @pl.when(me != to)
                def _():
                    sends[index][to] = raw[index][wants[to][0]]
                    copy_c(index, col, to, pair).start()

            hubs[index][col, pair] = raw[index][mine[0]]

    def pick(index):
        family, number = pieces[index]
        for half in range(2):
            for hub in range(pairs):

                @pl.when(me != 2 * hub_of(hub, levels) + half)
                def _():
                    copy_c(index, half, 2 * hub_of(hub, levels) + half, hub).wait_recv()

        for half in range(2):
            value = hubs[index][half, mine[1]]
            if family == "down":
                at = number + half * spans[index]
                x_part = r["x"][side, :, at : at + spans[index]]
                r["shrink_own"][:, :three] += contract(x_part, value)
            elif family == "small":
                r["small_all"][side, half] = value
            else:
                at = number + half * spans[index]
                r["up_all"][:, at : at + spans[index]] = value
        if family == "small":
            pair_small.start()

    done = {start_a: 0, start_b: 0, relay: 0, choose: 0, pick: 0}
    lags = {start_a: -AHEAD_A, start_b: -AHEAD_B, relay: 0, choose: LAG_C, pick: LAG_C + LAG_P}

    def up_to(action, index):
        while done[action] <= min(index, n - 1):
            action(done[action])
            done[action] += 1

    for index in range(AHEAD_A):
        up_to(start_a, index)
        if index < FIRST_B:
            up_to(start_b, index)
    for copy in (pair_tokens, pair_kv, pair_q, pair_wo):
        copy.start()
    meet()

    r["qacc"][...] = jnp.zeros_like(r["qacc"])
    r["kvacc"][...] = jnp.zeros_like(r["kvacc"])
    r["shrink_own"][...] = jnp.zeros_like(r["shrink_own"])
    r["up_maps"][...] = jnp.zeros_like(r["up_maps"])

    def base_block(number):
        tile = width // BASE_PIECES
        for half in range(2):
            cols = pl.ds(pl.multiple_of(number * tile, tile), tile)
            rows = pl.ds(pl.multiple_of(half * width + number * tile, tile), tile)
            x_block = r["x"][half, :, cols]
            r["qacc"][...] += mul(x_block, r["wq"][rows, :])
            r["kvacc"][...] += mul(x_block, r["wkv"][rows, :])

    last_down = max(i for i, p in enumerate(pieces) if p[0] == "down")
    base_done = 0
    steps = last_down + lags[pick] + 1
    first_base = steps - 5
    for number in range(steps):
        for action in (start_a, start_b, relay, choose, pick):
            if action is pick and done[pick] == 0 and number == lags[pick]:
                load_tokens.wait()
            limit = last_down + EARLY if action is choose else n
            up_to(action, min(number - lags[action], limit))
        if number == first_base:
            load_q.wait()
            load_kv.wait()
            for copy in (pair_tokens, pair_kv, pair_q):
                copy.wait_recv()
        if number >= first_base and base_done < BASE_PIECES:
            upto = min(BASE_PIECES, base_done + 2)

            @pl.loop(base_done, upto)
            def _(block):
                base_block(block)

            base_done = upto
    pair_shrink.start()

    def tail_point(point):
        up_to(relay, n)
        for at in TAIL:
            if at == point:
                up_to(choose, done[choose])

    tail_point(0)
    pair_small.wait_recv()
    lines = rank // 2
    for half in range(2):
        own = slice(half * q_here, (half + 1) * q_here)
        at = 2 * q_here + half * kv_here
        for part in range(2):
            small = r["small_all"][half, part]
            to = slice(part * lines, (part + 1) * lines)
            r["up_maps"][to, own] = small[:, :q_here]
            to_kv = slice((half + 1) * rank + part * lines, (half + 1) * rank + (part + 1) * lines)
            r["up_maps"][to_kv, at : at + kv_here] = small[:, q_here : q_here + kv_here]
            r["out_down"][to, own] = small[:, q_here + kv_here :]
    load_wo.wait()
    load_rope.wait()
    pair_wo.wait_recv()
    pair_shrink.wait_recv()
    tail_point(1)

    shrink = (r["shrink_own"][:, :three] + r["shrink_other"][:, :three]).astype(jnp.bfloat16)
    added = mul(shrink, r["up_maps"][...])
    rows_here = shrink.shape[0]
    kv = (r["kvacc"][...] + added[:, 2 * q_here :]).astype(jnp.bfloat16)
    cos_part, sin_part = r["rope_v"][0], r["rope_v"][1]

    def rotate(v):
        return (v * cos_part + pltpu.roll(v, HEAD_SIZE // 2, 1) * sin_part).astype(jnp.bfloat16)

    keys = rotate(kv[:, :HEAD_SIZE].astype(jnp.float32))
    values = kv[:, HEAD_SIZE:]
    tail_point(2)
    heads = 2 * q_here // HEAD_SIZE
    length = r["lengths"][0]
    line = lax.broadcasted_iota(jnp.int32, (rows_here, rows_here), 0)
    column = lax.broadcasted_iota(jnp.int32, (rows_here, rows_here), 1)
    allowed = (column <= line) & (column < length)
    for head in range(heads):
        at = slice(head * HEAD_SIZE, (head + 1) * HEAD_SIZE)
        query = rotate(r["qacc"][:, at] + added[:, at])
        scores = contract(query, keys) * HEAD_SIZE ** (-0.5)
        scores = jnp.where(allowed, scores, -1e30)
        highest = jnp.max(scores, axis=1, keepdims=True)
        expo = jnp.exp(scores - highest)
        weights = (expo / jnp.sum(expo, axis=1, keepdims=True)).astype(jnp.bfloat16)
        r["attended"][:, at] = mul(weights, values).astype(jnp.bfloat16)
        tail_point(3 + head)
    up_to(choose, n)
    low = contract(r["attended"][...], r["out_down"][...]).astype(jnp.bfloat16)
    tile = min(512, width)

    @pl.loop(0, width // tile)
    def _(block):
        cols = pl.ds(pl.multiple_of(block * tile, tile), tile)
        base = jnp.zeros((rows_here, tile), jnp.float32)
        for half in range(2):
            term = mul(r["attended"][:, half * q_here : (half + 1) * q_here], r["wo"][half, :, cols])
            base = base + term.astype(jnp.bfloat16).astype(jnp.float32)
        r["base"][:, cols] = base

    valid = lax.broadcasted_iota(jnp.int32, (rows_here, 1), 0) < length
    for index in range(last_down + 1, n):
        up_to(pick, index)
        for half in range(2):
            at = pieces[index][1] + half * spans[index]
            cols = slice(at, at + spans[index])
            total = r["base"][:, cols] + mul(low, r["up_all"][:, cols])
            r["out"][:, cols] = jnp.where(valid, total, 0.0).astype(jnp.bfloat16)

    for index in range(n):
        copy_a(index).wait_send()

        @pl.when(is_end)
        def _():
            copy_b_own(index).wait_send()
            copy_b_relay(index).wait_send()

        @pl.when(is_hub)
        def _():
            for to in range(2 * levels):

                @pl.when(me != to)
                def _():
                    copy_c(index, col, to, pair).wait_send()

    for copy in (pair_tokens, pair_q, pair_kv, pair_wo, pair_small, pair_shrink):
        copy.wait_send()


def local(tokens, qw, kvw, ow, adm, aqu, akv, aod, aou, req, pool, lengths):
    size = lax.axis_size("serve")
    count, rank, out_width = aou.shape
    rows, width = tokens.shape
    q_here, kv_here = qw.shape[1], kvw.shape[1]
    levels = size // 2
    small_width = q_here + kv_here + q_here
    pieces = [("small", 0, rank // 2, small_width)]
    for family, lines, whole, parts in (
        ("down", adm.shape[1], width, DOWN_PARTS),
        ("up", rank, out_width, UP_PARTS),
    ):
        unit = whole // (2 * sum(parts))
        for index, part in enumerate(parts):
            pieces.append((family, 2 * unit * sum(parts[:index]), lines, unit * part))
    bf16, f32 = jnp.bfloat16, jnp.float32
    scratch = {}
    for index, (_, _, lines, span) in enumerate(pieces):
        kinds = {
            "raw": (4 * count,), "give": (count,), "sends": (size,),
            "hubs": (2, levels // 2),
        }
        for kind, lead in kinds.items():
            scratch[f"{kind}{index}"] = pltpu.VMEM((*lead, lines, span), bf16)
    scratch.update(
        small_all=pltpu.VMEM((2, 2, rank // 2, small_width), bf16),
        up_all=pltpu.VMEM((rank, out_width), bf16),
        x=pltpu.VMEM((2, rows, width), bf16),
        wq=pltpu.VMEM((qw.shape[0], 2 * q_here), bf16),
        wkv=pltpu.VMEM((kvw.shape[0], 2 * kv_here), bf16),
        wo=pltpu.VMEM((2, ow.shape[0], out_width), bf16),
        rope_v=pltpu.VMEM((2, rows, HEAD_SIZE), f32),
        qacc=pltpu.VMEM((rows, 2 * q_here), f32),
        kvacc=pltpu.VMEM((rows, 2 * kv_here), f32),
        shrink_own=pltpu.VMEM((rows, 128), f32),
        shrink_other=pltpu.VMEM((rows, 128), f32),
        up_maps=pltpu.VMEM((3 * rank, 2 * q_here + 2 * kv_here), bf16),
        out_down=pltpu.VMEM((rank, 2 * q_here), bf16),
        attended=pltpu.VMEM((rows, 2 * q_here), bf16),
        req_s=pltpu.SMEM(req.shape, jnp.int32),
        pool_s=pltpu.SMEM(pool.shape, jnp.int32),
        met=pltpu.SemaphoreType.REGULAR,
        met_hubs=pltpu.SemaphoreType.REGULAR,
        table_sem=pltpu.SemaphoreType.DMA((2,)),
        load_sem=pltpu.SemaphoreType.DMA((5 + 2 * len(pieces) + 6,)),
        hop_send=pltpu.SemaphoreType.DMA((3, len(pieces))),
        hop_recv=pltpu.SemaphoreType.DMA((3, len(pieces))),
        c_send=pltpu.SemaphoreType.DMA((len(pieces), size)),
        c_recv=pltpu.SemaphoreType.DMA((len(pieces), 2, levels // 2)),
        base=pltpu.VMEM((rows, out_width), f32),
        pair_send=pltpu.SemaphoreType.DMA((6,)),
        pair_recv=pltpu.SemaphoreType.DMA((6,)),
    )
    operands = ["lengths", "req", "pool", "tokens", "qw", "kvw", "ow", "adm", "aqu", "akv", "aod", "aou", "rope"]
    plan = dict(
        names=operands + ["out"] + list(scratch),
        levels=levels, count=count, rank=rank, width=width, q_here=q_here, kv_here=kv_here,
        pieces=[piece[:2] for piece in pieces],
    )
    rope = jnp.asarray(rotary_tables(rows, HEAD_SIZE))
    arrays = (req, pool, tokens, qw, kvw, ow, adm, aqu, akv, aod, aou, rope)
    hbm = pl.BlockSpec(memory_space=pl.ANY)
    return pl.pallas_call(
        functools.partial(kernel, plan),
        out_shape=jax.ShapeDtypeStruct((rows, out_width), bf16),
        in_specs=[pl.BlockSpec(memory_space=pltpu.SMEM)] + [hbm] * len(arrays),
        out_specs=pl.BlockSpec(memory_space=pltpu.VMEM),
        scratch_shapes=list(scratch.values()),
        compiler_params=pltpu.CompilerParams(
            collective_id=0, has_side_effects=True, vmem_limit_bytes=50 * 1024 * 1024
        ),
        name="routed_attention",
    )(lengths, *[pltpu.with_memory_space_constraint(array, pltpu.HBM) for array in arrays])


def solution(mesh):
    placed = (
        P(("group", "serve"), "tensor"),
        P(None, "tensor"),
        P(None, "tensor"),
        P("tensor", None),
        P(("group", "serve"), None, "tensor"),
        P(("group", "serve"), None, "tensor"),
        P(("group", "serve"), None, "tensor"),
        P(("group", "serve"), None, "tensor"),
        P(("group", "serve"), None, "tensor"),
        P("group"),
        P("group"),
        P(("group", "serve")),
    )
    return jax.shard_map(
        local,
        mesh=mesh,
        in_specs=placed,
        out_specs=P(("group", "serve"), "tensor"),
        check_vma=False,
    )
```
